32 devices in a mesh: dp: 4 (over x, core), tensor: 8 (over z, y).
Axes of the slice: x: 2, y: 2, z: 4, core: 2. Of those that a mesh axis runs over, the one named last changes fastest.
Arguments:
- out_grad: bfloat16 [2, 320, 4096], P(None, 'dp', 'tensor'), may hold values from -0.3125 to 0.3125
- layer_input: bfloat16 [2, 320, 4096], P(None, 'dp', 'tensor'), may hold values from -8 to 8
- w_down: bfloat16 [16384, 4096], P('tensor'), may hold values from -0.046875 to 0.046875
- silu_gate: bfloat16 [2, 320, 16384], P(None, 'dp', 'tensor'), may hold values from -6 to 6
- up_proj: bfloat16 [2, 320, 16384], P(None, 'dp', 'tensor'), may hold values from -6 to 6
- slope_codes: int32 [2, 32, 16384], P(None, 'dp', 'tensor'), may hold values from 0 to 1073741823
Outputs:
- grad_down: bfloat16 [16384, 4096], P('tensor', 'dp')
- grad_gate: bfloat16 [4096, 16384], P('dp', 'tensor')
- grad_up: bfloat16 [4096, 16384], P('dp', 'tensor')
The draws below stay inside these ranges and needn't reach their ends.
Inputs may be any that keep to these rules, and one draw needn't show every extreme that they name: `slope_codes`: every word holds ten independent 3-bit codes; all eight codes occur.
All inputs are finite; a program needn't handle non-finite values.
Results may differ from the reference program's by a relative error of at most 0.018.
Values may be sent and summed in bfloat16 or wider, within the bound.
A program may use at most 128 MiB of HBM per device.

```python
import jax
import jax.numpy as jnp
from jax import lax

D = 4096
FF = 16384
MICRO = 2
TOK_MB = 80
TOKENS = 320
N_DP = 4


def plant(values, key, smallest, top_value):
    longest = values.shape.index(max(values.shape))
    spots = []
    for shift in (0, 1):
        where = [jax.random.randint(jax.random.fold_in(key, axis), (), 0, length) for axis, length in enumerate(values.shape)]
        where[longest] = (where[longest] + shift) % values.shape[longest]
        spots.append(tuple(where))
    return values.at[spots[0]].set(smallest).at[spots[1]].set(top_value)


def spiked(drawn, stream_key, source, target, shards_of, factor):
    def block_of(axis_at):
        return (jnp.arange(drawn.shape[axis_at]) // (drawn.shape[axis_at] // shards_of)).reshape((-1,) + (1,) * (drawn.ndim - 1 - axis_at))

    near = jax.random.permutation(stream_key, shards_of)[block_of(target)]
    other_side = (block_of(target) + shards_of // 2) % shards_of
    return jnp.where((block_of(source) == near) | (block_of(source) == other_side), factor * drawn, drawn)


def levels(rng, extent, split, smallest, largest):
    gain = 1.0
    for axis_at, blocks in split:
        draws = jax.random.uniform(jax.random.fold_in(jax.random.fold_in(rng, 6), axis_at), (blocks,), jnp.float32, smallest / len(split), largest / len(split))
        gain = gain * jnp.repeat(jnp.exp(draws), extent[axis_at] // blocks).reshape((-1,) + (1,) * (len(extent) - 1 - axis_at))
    return gain


def normal_values(stream_key, shape, scale, limit, cuts=(), kind=jnp.bfloat16):
    level = levels(stream_key, shape, cuts, -0.22, 0.18) if cuts else 1.0
    array = jax.random.normal(stream_key, shape, jnp.float32) * scale * level
    return jnp.minimum(jnp.maximum(array, -limit), limit).astype(kind)


def heavy_noise(rng, shape, spread, reach, split, heavy, held_as=jnp.bfloat16):
    values = spread * jax.random.normal(rng, shape, jnp.float32)
    if split:
        values = values * levels(rng, shape, split, -0.22, 0.18)
    return jnp.clip(spiked(values, jax.random.fold_in(rng, 3), *heavy), -reach, reach).astype(held_as)


def setup_inputs(seed: int = 0) -> dict:
    streams_of = jax.random.split(jax.random.key(seed), 7)
    return {
        "out_grad": heavy_noise(streams_of[0], (MICRO, TOKENS, D), (1.0 / (MICRO * TOKENS) ** 0.5), 0.3125, ((1, 4), (2, 8)), (1, 2, 8, 2.0)),
        "layer_input": heavy_noise(streams_of[1], (MICRO, TOKENS, D), 1.0, 8.0, ((1, 4), (2, 8)), (1, 2, 8, 2.0)),
        "w_down": normal_values(streams_of[2], (FF, D), FF ** -0.5, 0.046875, ((0, 8),)),
        "silu_gate": normal_values(streams_of[3], (MICRO, TOKENS, FF), 1.0, 6.0, ((1, 4), (2, 8))),
        "up_proj": normal_values(streams_of[4], (MICRO, TOKENS, FF), 1.0, 6.0, ((1, 4), (2, 8))),
        "slope_codes": plant(jax.random.randint(streams_of[5], (MICRO, TOKENS // 10, FF), 0, 1073741824), jax.random.fold_in(streams_of[5], 1), 0, 1073741823).astype(jnp.int32),
    }


SLOPE_LEVELS = (-0.09, 0.06, 0.22, 0.41, 0.6, 0.79, 0.96, 1.08)


def decode_slopes(packed):
    shifts = 3 * jnp.arange(10, dtype=jnp.int32)
    pieces = jnp.bitwise_and(jnp.right_shift(packed[..., None, :], shifts[:, None]), 7)
    pieces = pieces.reshape(packed.shape[:-2] + (packed.shape[-2] * 10, packed.shape[-1]))
    result = jnp.full(pieces.shape, SLOPE_LEVELS[0], jnp.float32)
    for symbol in range(1, 8):
        result = jnp.where(pieces == symbol, jnp.float32(SLOPE_LEVELS[symbol]), result)
    return result


def rounded(values):
    return lax.optimization_barrier(values.astype(jnp.bfloat16)).astype(jnp.float32)


def by_group(values):
    columns = values.shape[-1]
    shaped = values.reshape(MICRO, N_DP, TOK_MB, columns).transpose(1, 0, 2, 3)
    return shaped.reshape(N_DP, MICRO * TOK_MB, columns)


def reference(out_grad, layer_input, w_down, silu_gate, up_proj, slope_codes):
    slopes = decode_slopes(slope_codes)
    hidden_grad = jnp.dot(out_grad.reshape(-1, D), w_down.T, preferred_element_type=jnp.float32)
    hidden_grad = hidden_grad.reshape(MICRO, -1, FF)
    gate_act = silu_gate.astype(jnp.float32)
    up_value = up_proj.astype(jnp.float32)
    up_grad = (hidden_grad * gate_act).astype(jnp.bfloat16)
    gate_grad = (hidden_grad * up_value * slopes).astype(jnp.bfloat16)
    hidden = (gate_act * up_value).astype(jnp.bfloat16)

    def add_group(totals, pieces):
        inputs, output_rows, hidden_rows, gate_rows, up_rows = pieces
        gate_part = jnp.dot(inputs.T, gate_rows, preferred_element_type=jnp.float32)
        up_part = jnp.dot(inputs.T, up_rows, preferred_element_type=jnp.float32)
        down_part = jnp.dot(hidden_rows.T, output_rows, preferred_element_type=jnp.float32)
        return (totals[0] + rounded(gate_part), totals[1] + rounded(up_part), totals[2] + rounded(down_part)), None

    start_totals = (jnp.zeros((D, FF), jnp.float32), jnp.zeros((D, FF), jnp.float32), jnp.zeros((FF, D), jnp.float32))
    totals, unused = lax.scan(add_group, start_totals, (by_group(layer_input), by_group(out_grad), by_group(hidden), by_group(gate_grad), by_group(up_grad)))
    return (totals[2].astype(jnp.bfloat16), totals[0].astype(jnp.bfloat16), totals[1].astype(jnp.bfloat16))
```

```python
import functools

import jax
import jax.numpy as jnp
import numpy as np
from jax import lax
from jax.experimental import pallas as pl
from jax.experimental.pallas import tpu as pltpu
from jax.sharding import PartitionSpec as P

SLOPE_LEVELS = (-0.09, 0.06, 0.22, 0.41, 0.6, 0.79, 0.96, 1.08)
MESH = pl.DeviceIdType.MESH
EARLY = 4
HELD = 1
LATE = 8
TAIL = 2
SPLIT = 2
LAG = 3


def exchange(n_dp, n_t, out_hbm, in_hbm, silu_hbm, up_hbm, code_hbm, spread_hbm, w_hbm,
             down, gate_main, up_main, turned, gate_all, up_all,
             og, li, silu, up, codes, spread, w, slopes_up, acc, hid_all, xin, xout,
             l_sem, w_sem, u_send, u_recv, d_send, d_recv, y_send, y_recv,
             x_send, c_recv, zu_send, zd_send, cy_send, cy_recv, o_sem, o_send, o_recv,
             ax_send, ax_recv, ac_send, ac_recv):
    chips = n_dp // 2
    rows = n_t // 2
    ratio = n_t // n_dp
    tokens, cols = out_hbm.shape
    hidden, width = w_hbm.shape
    block = width // n_dp
    part = cols // SPLIT
    total = n_dp * tokens
    n_in, n_out = n_dp * SPLIT, (n_dp - 2) * SPLIT
    acts = (hid_all, gate_all, up_all)
    pieces = (EARLY, LATE, LATE)

    d = lax.axis_index("dp")
    t = lax.axis_index("tensor")
    q, c = d // 2, lax.rem(d, 2)
    z, y = t // 2, lax.rem(t, 2)
    partner = q * 2 + (1 - c)
    y_peer = z * 2 + (1 - y)
    z_up = lax.min(z + 1, rows - 1) * 2 + y
    z_down = lax.max(z - 1, 0) * 2 + y
    has_up, has_down = z + 1 < rows, z > 0
    owner = t // ratio
    if ratio == 2:
        in_chain = d >= 0
        has_side = d >= 0
        chain_col, side_col = y, 1 - y
    else:
        in_chain = lax.rem(d, 2) == y
        has_side = lax.rem(d, 2) != y
        chain_col, side_col = y * 0, y * 0
    in_head = (d * ratio) // 2
    out_head = lax.rem(in_head + rows // 2, rows)

    def chip_at(r):
        return lax.rem(q + r, chips) * 2 + c

    def group_from(r, core):
        return lax.rem(q + chips - r, chips) * 2 + core

    def span(index, size):
        return pl.ds(pl.multiple_of(index * size, 128), size)

    def remote(src, dst, send, recv, dp, tensor):
        return pltpu.make_async_remote_copy(
            src_ref=src, dst_ref=dst, send_sem=send, recv_sem=recv,
            device_id={"dp": dp, "tensor": tensor}, device_id_type=MESH)

    my_cols = og.at[:, span(t, cols)]
    loads = [
        pltpu.make_async_copy(out_hbm, my_cols, l_sem.at[0]),
        pltpu.make_async_copy(in_hbm, li, l_sem.at[1]),
        pltpu.make_async_copy(silu_hbm, silu, l_sem.at[2]),
        pltpu.make_async_copy(up_hbm, up, l_sem.at[3]),
        pltpu.make_async_copy(code_hbm, codes, l_sem.at[4]),
        pltpu.make_async_copy(spread_hbm, spread, l_sem.at[5]),
    ]
    for load in loads:
        load.start()

    fw = min(512, hidden)

    def w_copy(j):
        f = span(j, fw)
        return pltpu.make_async_copy(w_hbm.at[f], w.at[f], w_sem.at[j])

    for j in range(hidden // fw):
        w_copy(j).start()

    barrier = pltpu.get_barrier_semaphore()
    greet = [(d, y_peer), (partner, t)]
    greet += [(chip_at(r), t) for r in range(1, chips)]
    for r in range(1, chips):
        greet.append((lax.rem(q + r, chips) * 2 + 1 - c, t))
    for dp, tensor in greet:
        pl.semaphore_signal(barrier, inc=1, device_id={"dp": dp, "tensor": tensor}, device_id_type=MESH)

    @pl.when(has_up)
    def _():
        pl.semaphore_signal(barrier, inc=1, device_id={"dp": d, "tensor": z_up}, device_id_type=MESH)

    @pl.when(has_down)
    def _():
        pl.semaphore_signal(barrier, inc=1, device_id={"dp": d, "tensor": z_down}, device_id_type=MESH)

    pl.semaphore_wait(barrier, len(greet) + has_up.astype(jnp.int32) + has_down.astype(jnp.int32))

    def og_piece(row, col, h):
        return og.at[:, span((row * 2 + col) * SPLIT + h, part)]

    def up_copy(s, h):
        piece = og_piece(lax.max(z - s + 1, 0), y, h)
        return remote(piece, piece, u_send.at[s, h], u_recv.at[s, h], d, z_up)

    def down_copy(s, h):
        piece = og_piece(lax.min(z + s - 1, rows - 1), y, h)
        return remote(piece, piece, d_send.at[s, h], d_recv.at[s, h], d, z_down)

    def up_wait(s, h):
        piece = og_piece(lax.max(z - s, 0), y, h)
        return remote(piece, piece, u_send.at[s, h], u_recv.at[s, h], d, z_up)

    def down_wait(s, h):
        piece = og_piece(lax.min(z + s, rows - 1), y, h)
        return remote(piece, piece, d_send.at[s, h], d_recv.at[s, h], d, z_down)

    def across(row, h):
        piece = og_piece(row, y, h)
        return remote(piece, piece, y_send.at[row, h], y_recv.at[row, h], d, y_peer)

    def across_wait(row, h):
        piece = og_piece(row, 1 - y, h)
        return remote(piece, piece, y_send.at[row, h], y_recv.at[row, h], d, y_peer)

    loads[0].wait()
    for h in range(SPLIT):
        across(z, h).start()

        @pl.when(has_up)
        def _():
            up_copy(1, h).start()

        @pl.when(has_down)
        def _():
            down_copy(1, h).start()

    def in_piece(group, col, h):
        return xin.at[group, :, span(col * SPLIT + h, part)]

    def out_piece(group, col, h):
        return xout.at[group, :, span(col * SPLIT + h, part)]

    in_slot = (lax.rem(owner // 2 + chips - q, chips) * 2 + c) * SPLIT

    def li_remote(h):
        return remote(li.at[:, h * part:(h + 1) * part], in_piece(d, chain_col_of(t), h),
                      x_send.at[h], c_recv.at[in_slot + h], owner, t)

    def li_local(h):
        return pltpu.make_async_copy(li.at[:, h * part:(h + 1) * part], in_piece(d, chain_col_of(t), h),
                                     c_recv.at[in_slot + h])

    def chain_col_of(tensor):
        return lax.rem(tensor, 2) if ratio == 2 else tensor * 0

    loads[1].wait()
    owned = owner == d

    @pl.when(owned)
    def _():
        for h in range(SPLIT):
            li_local(h).start()

    @pl.when(jnp.logical_not(owned))
    def _():
        for h in range(SPLIT):
            li_remote(h).start()

    far_row = lax.rem(z + rows // 2, rows)
    far_owner = (far_row * 2 + y) // ratio
    crosses = far_owner // 2 != q
    far_dist = lax.max(lax.rem(far_owner // 2 + chips - q, chips), 1)
    out_slot = n_in + ((far_dist - 1) * 2 + c) * SPLIT

    def og_far(h):
        return remote(og_piece(far_row, y, h), out_piece(d, chain_col_of(t), h),
                      x_send.at[SPLIT + h], c_recv.at[out_slot + h], far_owner, t)

    def f_part(a, j):
        return span(j, hidden // pieces[a])

    def own_chip(a, j, r):
        own = acts[a].at[d, :, f_part(a, j)]
        return remote(own, own, ax_send.at[a, r - 1, j], ax_recv.at[a, r - 1, j], chip_at(r), t)

    def own_core(a, j):
        own = acts[a].at[d, :, f_part(a, j)]
        return remote(own, own, ac_send.at[a, 0, j], ac_recv.at[a, 0, j], partner, t)

    def pass_core(a, j, r):
        land = acts[a].at[group_from(r, c), :, f_part(a, j)]
        return remote(land, land, ac_send.at[a, r, j], ac_recv.at[a, r, j], partner, t)

    def chip_wait(a, j, r):
        land = acts[a].at[group_from(r, c), :, f_part(a, j)]
        return remote(land, land, ax_send.at[a, r - 1, j], ax_recv.at[a, r - 1, j], partner, t)

    def core_wait(a, j, r):
        land = acts[a].at[group_from(r, 1 - c), :, f_part(a, j)]
        return remote(land, land, ac_send.at[a, r, j], ac_recv.at[a, r, j], partner, t)

    def send_own(a, j):
        for r in range(1, chips):
            own_chip(a, j, r).start()
        own_core(a, j).start()

    def relay(a, j):
        for r in range(1, chips):
            chip_wait(a, j, r).wait_recv()
            pass_core(a, j, r).start()

    loads[2].wait()
    loads[3].wait()

    def early(j, carry):
        f = f_part(0, j)
        hid_all[d, :, f] = (silu[:, f].astype(jnp.float32) * up[:, f].astype(jnp.float32)).astype(jnp.bfloat16)

        @pl.when(j < EARLY - HELD)
        def _():
            send_own(0, j)
        return carry

    lax.fori_loop(0, EARLY, early, 0)

    loads[4].wait()
    loads[5].wait()
    acc[...] = jnp.zeros_like(acc)

    def decode(j, carry):
        f = span(j, fw)
        words = codes[:, f]
        symbols = jnp.dot(
            spread[...],
            jnp.concatenate([((words >> (3 * k)) & 7).astype(jnp.float32).astype(jnp.bfloat16) for k in range(10)], axis=0),
            preferred_element_type=jnp.float32)
        slopes = jnp.full(symbols.shape, SLOPE_LEVELS[0], jnp.float32)
        for s in range(1, 8):
            slopes = jnp.where(symbols > s - 0.5, jnp.float32(SLOPE_LEVELS[s]), slopes)
        slopes_up[:, f] = up[:, f].astype(jnp.float32) * slopes
        return carry

    lax.fori_loop(0, hidden // fw, decode, 0)

    def unit(i):
        h, u = lax.rem(i, SPLIT), i // SPLIT
        return lax.rem(u, 2), u // 2, h

    def in_ref(i, col):
        core, r, h = unit(i)
        return in_piece(group_from(r, core), col, h)

    def out_ref(i, col):
        core, r, h = unit(i)
        return out_piece(group_from(r + 1, core), col, h)

    def chain(i, base, ref):
        piece = ref(i, chain_col)
        n = base + i
        return (remote(piece, piece, zu_send.at[n], c_recv.at[n], d, z_up),
                remote(piece, piece, zd_send.at[n], c_recv.at[n], d, z_down),
                remote(piece, piece, cy_send.at[n], cy_recv.at[n], d, y_peer))

    def goes(head):
        return (jnp.logical_and(in_chain, jnp.logical_and(z >= head, has_up)),
                jnp.logical_and(in_chain, jnp.logical_and(z <= head, has_down)))

    def chain_step(i, base, ref, head):
        up_next, down_next, side = chain(i, base, ref)
        go_up, go_down = goes(head)
        up_next.wait_recv()

        @pl.when(go_up)
        def _():
            up_next.start()

        @pl.when(go_down)
        def _():
            down_next.start()

        side.start()

    in_far = lax.max(z - in_head, in_head - z)
    out_far = lax.max(z - out_head, out_head - z)
    at_in_head = jnp.logical_and(in_chain, in_far == 0)

    def matmul_piece(piece):
        k = span(piece, cols)

        def f_step(j, carry):
            f = span(j, fw)
            acc[:, f] += lax.dot_general(og[:, k], w[f, k], (((1,), (1,)), ((), ())),
                                         preferred_element_type=jnp.float32)
            return carry

        lax.fori_loop(0, hidden // fw, f_step, 0)

    def gather(s, carry):
        below, above = z >= s, z + s < rows
        for h in range(SPLIT):
            @pl.when(below)
            def _():
                up_wait(s, h).wait_recv()

                @pl.when(has_up)
                def _():
                    up_copy(s + 1, h).start()

                across(lax.max(z - s, 0), h).start()

            @pl.when(above)
            def _():
                down_wait(s, h).wait_recv()

                @pl.when(has_down)
                def _():
                    down_copy(s + 1, h).start()

                across(lax.min(z + s, rows - 1), h).start()

        @pl.when(s == rows // 2)
        def _():
            @pl.when(crosses)
            def _():
                for h in range(SPLIT):
                    og_far(h).start()

            for j in range(EARLY - HELD, EARLY):
                send_own(0, j)

        @pl.when(s == 1)
        def _():
            for j in range(hidden // fw):
                w_copy(j).wait()

        @pl.when(jnp.logical_and(s == rows - 1, at_in_head))
        def _():
            def start(i, carry):
                chain_step(i, 0, in_ref, in_head)
                return carry

            lax.fori_loop(0, n_in, start, 0)

        def piece_step(k, carry):
            side = k >= 3
            dist = jnp.where(k == 0, 0, jnp.where(side, s - 1, s))
            down_side = jnp.logical_or(k == 1, k == 3)
            row = jnp.where(down_side, z - dist, z + dist)
            wanted = jnp.where(k == 0, s == 1, jnp.logical_or(dist > 0, down_side))
            valid = jnp.logical_and(wanted, jnp.logical_and(row >= 0, row < rows))

            @pl.when(valid)
            def _():
                @pl.when(side)
                def _():
                    for h in range(SPLIT):
                        across_wait(row, h).wait_recv()

                matmul_piece(row * 2 + jnp.where(side, 1 - y, y))
            return carry

        lax.fori_loop(0, 5, piece_step, 0)
        return carry

    lax.fori_loop(1, rows + 1, gather, 0)

    o_own = pltpu.make_async_copy(og.at[:, span(d, block)], xout.at[d], o_sem)
    o_own.start()
    o_other = remote(og.at[:, span(partner, block)], xout.at[d], o_send, o_recv, partner, t)
    o_other.start()

    def late(j):
        f = f_part(1, j)
        grad = acc[:, f]
        gate_all[d, :, f] = (grad * slopes_up[:, f]).astype(jnp.bfloat16)
        up_all[d, :, f] = (grad * silu[:, f].astype(jnp.float32)).astype(jnp.bfloat16)
        send_own(1, j)
        send_own(2, j)

    steps = max(n_in + rows - 2, n_out + LAG + rows - 1, LATE)

    def wave(s, carry):
        @pl.when(s < LATE)
        def _():
            late(s)

        i = s - (in_far - 1)

        @pl.when(jnp.logical_and(jnp.logical_and(in_chain, in_far > 0), jnp.logical_and(i >= 0, i < n_in)))
        def _():
            chain_step(i, 0, in_ref, in_head)

        o = s - LAG - out_far

        @pl.when(jnp.logical_and(in_chain, jnp.logical_and(o >= 0, o < n_out)))
        def _():
            chain_step(o, n_in, out_ref, out_head)
        return carry

    lax.fori_loop(0, steps, wave, 0)

    def hidden_relay(j, carry):
        relay(0, j)
        return carry

    lax.fori_loop(0, EARLY, hidden_relay, 0)

    def side_wait(i, base, ref):
        @pl.when(has_side)
        def _():
            piece = ref(i, side_col)
            remote(piece, piece, cy_send.at[base + i], cy_recv.at[base + i], d, y_peer).wait_recv()

    def out_side(i, carry):
        side_wait(i, n_in, out_ref)
        return carry

    def in_side(i, carry):
        side_wait(i, 0, in_ref)
        return carry

    lax.fori_loop(0, n_out, out_side, 0)
    o_own.wait()
    o_other.wait()

    def from_partner(a):
        def step(j, carry):
            for r in range(chips):
                core_wait(a, j, r).wait_recv()
            return carry
        return step

    lax.fori_loop(0, EARLY, from_partner(0), 0)

    def product(left, right):
        return jnp.dot(left, right, preferred_element_type=jnp.float32).astype(jnp.bfloat16)

    def down_step(j, carry):
        f = span(j, fw)
        down[f, :] = product(hid_all[:, :, f].reshape(total, fw).T, xout[...].reshape(total, block))
        return carry

    lax.fori_loop(0, hidden // fw, down_step, 0)
    lax.fori_loop(0, n_in, in_side, 0)
    turned[...] = xin[...].reshape(total, block).T

    def main_step(j, carry):
        relay(1, j)
        relay(2, j)

        @pl.when(j > 0)
        def _():
            for a in (1, 2):
                from_partner(a)(j - 1, 0)
            f = f_part(1, j - 1)
            size = hidden // LATE
            gate_main[:, f] = product(turned[...], gate_all[:, :, f].reshape(total, size))
            up_main[:, f] = product(turned[...], up_all[:, :, f].reshape(total, size))
        return carry

    lax.fori_loop(0, LATE - TAIL + 1, main_step, 0)
    for j in range(LATE - TAIL + 1, LATE):
        relay(1, j)
        relay(2, j)

    def gather_end(s, carry):
        for h in range(SPLIT):
            @pl.when(jnp.logical_and(has_up, z >= s - 1))
            def _():
                up_copy(s, h).wait_send()

            @pl.when(jnp.logical_and(has_down, z + s - 1 < rows))
            def _():
                down_copy(s, h).wait_send()

            across(s - 1, h).wait_send()
        return carry

    lax.fori_loop(1, rows + 1, gather_end, 0)

    @pl.when(jnp.logical_not(owned))
    def _():
        for h in range(SPLIT):
            li_remote(h).wait_send()

    @pl.when(crosses)
    def _():
        for h in range(SPLIT):
            og_far(h).wait_send()

    def chain_end(i, base, ref, head):
        up_next, down_next, side = chain(i, base, ref)
        go_up, go_down = goes(head)

        @pl.when(go_up)
        def _():
            up_next.wait_send()

        @pl.when(go_down)
        def _():
            down_next.wait_send()

        @pl.when(in_chain)
        def _():
            side.wait_send()

    def in_end(i, carry):
        chain_end(i, 0, in_ref, in_head)
        return carry

    def out_end(i, carry):
        chain_end(i, n_in, out_ref, out_head)
        return carry

    lax.fori_loop(0, n_in, in_end, 0)
    lax.fori_loop(0, n_out, out_end, 0)

    def sent(a):
        def step(j, carry):
            own_core(a, j).wait_send()
            for r in range(1, chips):
                own_chip(a, j, r).wait_send()
                pass_core(a, j, r).wait_send()
            return carry
        return step

    for a in range(3):
        lax.fori_loop(0, pieces[a], sent(a), 0)
    for a in (1, 2):
        lax.fori_loop(LATE - TAIL, LATE, from_partner(a), 0)


def finish(down_in, gate_in, up_in, turned, gate_all, up_all, down_out, gate_out, up_out, gate_tail, up_tail, sems):
    n_dp, tokens, hidden = gate_all.shape
    total = n_dp * tokens
    main = gate_in.shape[1]
    size = (hidden - main) // TAIL
    copies = [
        pltpu.make_async_copy(down_in, down_out, sems.at[0]),
        pltpu.make_async_copy(gate_in, gate_out.at[:, :main], sems.at[1]),
        pltpu.make_async_copy(up_in, up_out.at[:, :main], sems.at[2]),
    ]
    for copy in copies:
        copy.start()
    for j in range(TAIL):
        f = slice(main + j * size, main + (j + 1) * size)
        for k, (acts, tail, out) in enumerate(((gate_all, gate_tail, gate_out), (up_all, up_tail, up_out))):
            tail[j] = jnp.dot(turned[...], acts[:, :, f].reshape(total, size),
                              preferred_element_type=jnp.float32).astype(jnp.bfloat16)
            copies.append(pltpu.make_async_copy(tail.at[j], out.at[:, f], sems.at[3 + j * 2 + k]))
            copies[-1].start()
    for copy in copies:
        copy.wait()


def shards(n_dp, n_t, out_grad, layer_input, w_down, silu_gate, up_proj, slope_codes):
    hidden, width = w_down.shape
    cols = out_grad.shape[2]
    tokens = out_grad.shape[0] * out_grad.shape[1]
    chips, rows, block = n_dp // 2, n_t // 2, width // n_dp
    words = tokens // 10
    total = n_dp * tokens
    row, col = np.arange(tokens)[:, None], np.arange(tokens)[None, :]
    spread = jnp.asarray(col == (row % 10) * words + row // 10, jnp.bfloat16)
    units = (2 * n_dp - 2) * SPLIT
    far = chips - 1
    bf16 = jnp.bfloat16
    dma = pltpu.SemaphoreType.DMA
    vmem = pl.BlockSpec(memory_space=pltpu.VMEM)
    anywhere = pl.BlockSpec(memory_space=pl.ANY)
    main = hidden // LATE * (LATE - TAIL)
    flops = 2 * tokens * hidden * width + 5 * total * hidden * block
    held = pl.pallas_call(
        functools.partial(exchange, n_dp, n_t),
        out_shape=tuple(pltpu.VMEM(shape, bf16) for shape in (
            (hidden, block), (block, main), (block, main), (block, total),
            (n_dp, tokens, hidden), (n_dp, tokens, hidden))),
        in_specs=[anywhere] * 7,
        out_specs=[vmem] * 6,
        scratch_shapes=[
            pltpu.VMEM((tokens, width), bf16),
            pltpu.VMEM((tokens, cols), bf16),
            pltpu.VMEM((tokens, hidden), bf16),
            pltpu.VMEM((tokens, hidden), bf16),
            pltpu.VMEM((words, hidden), jnp.int32),
            pltpu.VMEM((tokens, tokens), bf16),
            pltpu.VMEM((hidden, width), bf16),
            pltpu.VMEM((tokens, hidden), jnp.float32),
            pltpu.VMEM((tokens, hidden), jnp.float32),
            pltpu.VMEM((n_dp, tokens, hidden), bf16),
            pltpu.VMEM((n_dp, tokens, block), bf16),
            pltpu.VMEM((n_dp, tokens, block), bf16),
            dma((6,)), dma((max(1, hidden // min(512, hidden)),)),
            dma((rows + 2, SPLIT)), dma((rows + 2, SPLIT)), dma((rows + 2, SPLIT)), dma((rows + 2, SPLIT)),
            dma((rows, SPLIT)), dma((rows, SPLIT)),
            dma((2 * SPLIT,)), dma((units,)), dma((units,)), dma((units,)), dma((units,)), dma((units,)),
            dma, dma, dma,
            dma((3, far, LATE)), dma((3, far, LATE)), dma((3, chips, LATE)), dma((3, chips, LATE)),
        ],
        compiler_params=pltpu.CompilerParams(
            collective_id=0, has_side_effects=True, vmem_limit_bytes=38 * 1024 * 1024),
        cost_estimate=pl.CostEstimate(flops=flops, bytes_accessed=20_000_000, transcendentals=0),
    )(
        out_grad.reshape(tokens, cols), layer_input.reshape(tokens, cols),
        silu_gate.reshape(tokens, hidden), up_proj.reshape(tokens, hidden),
        slope_codes.reshape(words, hidden), spread, w_down,
    )
    across = jax.ShapeDtypeStruct((block, hidden), bf16)
    size = hidden // LATE
    return pl.pallas_call(
        finish,
        out_shape=(jax.ShapeDtypeStruct((hidden, block), bf16), across, across),
        in_specs=[vmem] * 6,
        out_specs=[anywhere] * 3,
        scratch_shapes=[
            pltpu.VMEM((TAIL, block, size), bf16), pltpu.VMEM((TAIL, block, size), bf16), dma((3 + 2 * TAIL,))],
        compiler_params=pltpu.CompilerParams(vmem_limit_bytes=12 * 1024 * 1024),
    )(*(pltpu.with_memory_space_constraint(value, pltpu.VMEM) for value in held))


def solution(mesh):
    n_dp, n_t = mesh.shape["dp"], mesh.shape["tensor"]
    return jax.shard_map(
        functools.partial(shards, n_dp, n_t),
        mesh=mesh,
        in_specs=(
            P(None, "dp", "tensor"),
            P(None, "dp", "tensor"),
            P("tensor", None),
            P(None, "dp", "tensor"),
            P(None, "dp", "tensor"),
            P(None, "dp", "tensor"),
        ),
        out_specs=(P("tensor", "dp"), P("dp", "tensor"), P("dp", "tensor")),
        check_vma=False,
    )
```

```python
import functools

import jax
import jax.numpy as jnp
import numpy as np
from jax import lax
from jax.experimental import pallas as pl
from jax.experimental.pallas import tpu as pltpu
from jax.sharding import PartitionSpec as P

SLOPE_LEVELS = (-0.09, 0.06, 0.22, 0.41, 0.6, 0.79, 0.96, 1.08)
MESH = pl.DeviceIdType.MESH
EARLY = 4
HELD = 1
LATE = 8
AHEAD = 3
TAIL = 2
SPLIT = 2
LAG = 2


def exchange(n_dp, n_t, out_hbm, in_hbm, silu_hbm, up_hbm, code_hbm, spread_hbm, w_hbm,
             down, gate_main, up_main, turned, both_all,
             og, li, silu, up, codes, spread, w, slopes_up, acc, hid_all, xin, xout,
             l_sem, w_sem, u_send, u_recv, d_send, d_recv, y_send, y_recv,
             x_send, c_recv, zu_send, zd_send, cy_send, cy_recv, o_sem, o_send, o_recv,
             ax_send, ax_recv, ac_send, ac_recv):
    chips = n_dp // 2
    rows = n_t // 2
    ratio = n_t // n_dp
    tokens, cols = out_hbm.shape
    hidden, width = w_hbm.shape
    block = width // n_dp
    part = cols // SPLIT
    total = n_dp * tokens
    n_in, n_out = n_dp * SPLIT, (n_dp - 2) * SPLIT
    acts = (hid_all, both_all)
    pieces = (EARLY, LATE)
    size = hidden // LATE

    d = lax.axis_index("dp")
    t = lax.axis_index("tensor")
    q, c = d // 2, lax.rem(d, 2)
    z, y = t // 2, lax.rem(t, 2)
    partner = q * 2 + (1 - c)
    y_peer = z * 2 + (1 - y)
    z_up = lax.min(z + 1, rows - 1) * 2 + y
    z_down = lax.max(z - 1, 0) * 2 + y
    has_up, has_down = z + 1 < rows, z > 0
    owner = t // ratio
    if ratio == 2:
        in_chain = d >= 0
        has_side = d >= 0
        chain_col, side_col = y, 1 - y
    else:
        in_chain = lax.rem(d, 2) == y
        has_side = lax.rem(d, 2) != y
        chain_col, side_col = y * 0, y * 0
    in_head = (d * ratio) // 2
    out_head = lax.rem(in_head + rows // 2, rows)

    def chip_at(r):
        return lax.rem(q + r, chips) * 2 + c

    def group_from(r, core):
        return lax.rem(q + chips - r, chips) * 2 + core

    def span(index, size):
        return pl.ds(pl.multiple_of(index * size, 128), size)

    def remote(src, dst, send, recv, dp, tensor):
        return pltpu.make_async_remote_copy(
            src_ref=src, dst_ref=dst, send_sem=send, recv_sem=recv,
            device_id={"dp": dp, "tensor": tensor}, device_id_type=MESH)

    my_cols = og.at[:, span(t, cols)]
    loads = [
        pltpu.make_async_copy(out_hbm, my_cols, l_sem.at[0]),
        pltpu.make_async_copy(in_hbm, li, l_sem.at[1]),
        pltpu.make_async_copy(silu_hbm, silu, l_sem.at[2]),
        pltpu.make_async_copy(up_hbm, up, l_sem.at[3]),
        pltpu.make_async_copy(code_hbm, codes, l_sem.at[4]),
        pltpu.make_async_copy(spread_hbm, spread, l_sem.at[5]),
    ]
    for load in loads:
        load.start()

    fw = min(512, hidden)

    def w_copy(j):
        f = span(j, fw)
        return pltpu.make_async_copy(w_hbm.at[f], w.at[f], w_sem.at[j])

    barrier = pltpu.get_barrier_semaphore()
    greet = [(d, y_peer), (partner, t)]
    greet += [(chip_at(r), t) for r in range(1, chips)]
    for r in range(1, chips):
        greet.append((lax.rem(q + r, chips) * 2 + 1 - c, t))
    for dp, tensor in greet:
        pl.semaphore_signal(barrier, inc=1, device_id={"dp": dp, "tensor": tensor}, device_id_type=MESH)

    @pl.when(has_up)
    def _():
        pl.semaphore_signal(barrier, inc=1, device_id={"dp": d, "tensor": z_up}, device_id_type=MESH)

    @pl.when(has_down)
    def _():
        pl.semaphore_signal(barrier, inc=1, device_id={"dp": d, "tensor": z_down}, device_id_type=MESH)

    pl.semaphore_wait(barrier, len(greet) + has_up.astype(jnp.int32) + has_down.astype(jnp.int32))

    def og_piece(row, col, h):
        return og.at[:, span((row * 2 + col) * SPLIT + h, part)]

    def up_copy(s, h):
        piece = og_piece(lax.max(z - s + 1, 0), y, h)
        return remote(piece, piece, u_send.at[s, h], u_recv.at[s, h], d, z_up)

    def down_copy(s, h):
        piece = og_piece(lax.min(z + s - 1, rows - 1), y, h)
        return remote(piece, piece, d_send.at[s, h], d_recv.at[s, h], d, z_down)

    def up_wait(s, h):
        piece = og_piece(lax.max(z - s, 0), y, h)
        return remote(piece, piece, u_send.at[s, h], u_recv.at[s, h], d, z_up)

    def down_wait(s, h):
        piece = og_piece(lax.min(z + s, rows - 1), y, h)
        return remote(piece, piece, d_send.at[s, h], d_recv.at[s, h], d, z_down)

    def across(row, h):
        piece = og_piece(row, y, h)
        return remote(piece, piece, y_send.at[row, h], y_recv.at[row, h], d, y_peer)

    def across_wait(row, h):
        piece = og_piece(row, 1 - y, h)
        return remote(piece, piece, y_send.at[row, h], y_recv.at[row, h], d, y_peer)

    loads[0].wait()
    for h in range(SPLIT):
        across(z, h).start()

        @pl.when(has_up)
        def _():
            up_copy(1, h).start()

        @pl.when(has_down)
        def _():
            down_copy(1, h).start()

    def in_piece(group, col, h):
        return xin.at[group, :, span(col * SPLIT + h, part)]

    def out_piece(group, col, h):
        return xout.at[group, :, span(col * SPLIT + h, part)]

    in_slot = (lax.rem(owner // 2 + chips - q, chips) * 2 + c) * SPLIT

    def li_remote(h):
        return remote(li.at[:, h * part:(h + 1) * part], in_piece(d, chain_col_of(t), h),
                      x_send.at[h], c_recv.at[in_slot + h], owner, t)

    def li_local(h):
        return pltpu.make_async_copy(li.at[:, h * part:(h + 1) * part], in_piece(d, chain_col_of(t), h),
                                     c_recv.at[in_slot + h])

    def chain_col_of(tensor):
        return lax.rem(tensor, 2) if ratio == 2 else tensor * 0

    loads[1].wait()
    owned = owner == d

    @pl.when(owned)
    def _():
        for h in range(SPLIT):
            li_local(h).start()

    @pl.when(jnp.logical_not(owned))
    def _():
        for h in range(SPLIT):
            li_remote(h).start()

    far_row = lax.rem(z + rows // 2, rows)
    far_owner = (far_row * 2 + y) // ratio
    crosses = far_owner // 2 != q
    far_dist = lax.max(lax.rem(far_owner // 2 + chips - q, chips), 1)
    out_slot = n_in + ((far_dist - 1) * 2 + c) * SPLIT

    def og_far(h):
        return remote(og_piece(far_row, y, h), out_piece(d, chain_col_of(t), h),
                      x_send.at[SPLIT + h], c_recv.at[out_slot + h], far_owner, t)

    def f_part(a, j):
        return span(j, acts[a].shape[2] // pieces[a])

    def own_chip(a, j, r):
        own = acts[a].at[d, :, f_part(a, j)]
        return remote(own, own, ax_send.at[a, r - 1, j], ax_recv.at[a, r - 1, j], chip_at(r), t)

    def own_core(a, j):
        own = acts[a].at[d, :, f_part(a, j)]
        return remote(own, own, ac_send.at[a, 0, j], ac_recv.at[a, 0, j], partner, t)

    def pass_core(a, j, r):
        land = acts[a].at[group_from(r, c), :, f_part(a, j)]
        return remote(land, land, ac_send.at[a, r, j], ac_recv.at[a, r, j], partner, t)

    def chip_wait(a, j, r):
        land = acts[a].at[group_from(r, c), :, f_part(a, j)]
        return remote(land, land, ax_send.at[a, r - 1, j], ax_recv.at[a, r - 1, j], partner, t)

    def core_wait(a, j, r):
        land = acts[a].at[group_from(r, 1 - c), :, f_part(a, j)]
        return remote(land, land, ac_send.at[a, r, j], ac_recv.at[a, r, j], partner, t)

    def send_own(a, j):
        for r in range(1, chips):
            own_chip(a, j, r).start()
        own_core(a, j).start()

    def relay(a, j):
        for r in range(1, chips):
            chip_wait(a, j, r).wait_recv()
            pass_core(a, j, r).start()

    loads[2].wait()
    loads[3].wait()

    def early(j, carry):
        f = f_part(0, j)
        hid_all[d, :, f] = (silu[:, f].astype(jnp.float32) * up[:, f].astype(jnp.float32)).astype(jnp.bfloat16)

        @pl.when(j < EARLY - HELD)
        def _():
            send_own(0, j)
        return carry

    lax.fori_loop(0, EARLY, early, 0)

    for j in range(hidden // fw):
        w_copy(j).start()
    loads[4].wait()
    loads[5].wait()
    acc[...] = jnp.zeros_like(acc)

    def decode(j, carry):
        f = span(j, fw)
        words = codes[:, f]
        symbols = jnp.dot(
            spread[...],
            jnp.concatenate([((words >> (3 * k)) & 7).astype(jnp.float32).astype(jnp.bfloat16) for k in range(10)], axis=0),
            preferred_element_type=jnp.float32)
        slopes = jnp.full(symbols.shape, SLOPE_LEVELS[0], jnp.float32)
        for s in range(1, 8):
            slopes = jnp.where(symbols > s - 0.5, jnp.float32(SLOPE_LEVELS[s]), slopes)
        slopes_up[:, f] = up[:, f].astype(jnp.float32) * slopes
        return carry

    lax.fori_loop(0, hidden // fw, decode, 0)

    def unit(i):
        h, u = lax.rem(i, SPLIT), i // SPLIT
        return lax.rem(u, 2), u // 2, h

    def in_ref(i, col):
        core, r, h = unit(i)
        return in_piece(group_from(r, core), col, h)

    def out_ref(i, col):
        core, r, h = unit(i)
        return out_piece(group_from(r + 1, core), col, h)

    def chain(i, base, ref):
        piece = ref(i, chain_col)
        n = base + i
        return (remote(piece, piece, zu_send.at[n], c_recv.at[n], d, z_up),
                remote(piece, piece, zd_send.at[n], c_recv.at[n], d, z_down),
                remote(piece, piece, cy_send.at[n], cy_recv.at[n], d, y_peer))

    def goes(head):
        return (jnp.logical_and(in_chain, jnp.logical_and(z >= head, has_up)),
                jnp.logical_and(in_chain, jnp.logical_and(z <= head, has_down)))

    def chain_step(i, base, ref, head):
        up_next, down_next, side = chain(i, base, ref)
        go_up, go_down = goes(head)
        up_next.wait_recv()

        @pl.when(go_up)
        def _():
            up_next.start()

        @pl.when(go_down)
        def _():
            down_next.start()

        side.start()

    def head_rows(i, carry):
        up_next, down_next, side = chain(i, 0, in_ref)
        go_up, go_down = goes(in_head)
        up_next.wait_recv()

        @pl.when(go_up)
        def _():
            up_next.start()

        @pl.when(go_down)
        def _():
            down_next.start()
        return carry

    def head_side(i, carry):
        chain(i, 0, in_ref)[2].start()
        return carry

    in_far = lax.max(z - in_head, in_head - z)
    out_far = lax.max(z - out_head, out_head - z)
    at_in_head = jnp.logical_and(in_chain, in_far == 0)

    def matmul_piece(piece):
        k = span(piece, cols)
        acc[...] += lax.dot_general(og[:, k], w[:, k], (((1,), (1,)), ((), ())),
                                    preferred_element_type=jnp.float32)

    def wave_step(s):
        i = s - 2 * (in_far - 1)

        @pl.when(jnp.logical_and(jnp.logical_and(in_chain, in_far > 0), jnp.logical_and(i >= 0, i < n_in)))
        def _():
            chain_step(i, 0, in_ref, in_head)

        o = s - LAG - 2 * out_far

        @pl.when(jnp.logical_and(in_chain, jnp.logical_and(o >= 0, o < n_out)))
        def _():
            chain_step(o, n_in, out_ref, out_head)

    def gather(s, carry):
        below, above = z >= s, z + s < rows
        for h in range(SPLIT):
            @pl.when(below)
            def _():
                up_wait(s, h).wait_recv()

                @pl.when(has_up)
                def _():
                    up_copy(s + 1, h).start()

                across(lax.max(z - s, 0), h).start()

            @pl.when(above)
            def _():
                down_wait(s, h).wait_recv()

                @pl.when(has_down)
                def _():
                    down_copy(s + 1, h).start()

                across(lax.min(z + s, rows - 1), h).start()

        @pl.when(s == rows // 2)
        def _():
            @pl.when(crosses)
            def _():
                for h in range(SPLIT):
                    og_far(h).start()

            for j in range(EARLY - HELD, EARLY):
                send_own(0, j)

            @pl.when(at_in_head)
            def _():
                lax.fori_loop(0, n_in, head_rows, 0)

        @pl.when(s == 1)
        def _():
            for j in range(hidden // fw):
                w_copy(j).wait()

        @pl.when(jnp.logical_and(s == rows - 1, at_in_head))
        def _():
            lax.fori_loop(0, n_in, head_side, 0)

        @pl.when(s >= rows)
        def _():
            wave_step(s - rows)

        def piece_step(k, carry):
            side = k >= 3
            dist = jnp.where(k == 0, 0, jnp.where(side, s - 2, s))
            down_side = jnp.logical_or(k == 1, k == 3)
            row = jnp.where(down_side, z - dist, z + dist)
            wanted = jnp.where(k == 0, s == 1, jnp.logical_or(dist > 0, jnp.logical_and(dist == 0, down_side)))
            valid = jnp.logical_and(wanted, jnp.logical_and(row >= 0, row < rows))

            @pl.when(valid)
            def _():
                @pl.when(side)
                def _():
                    for h in range(SPLIT):
                        across_wait(row, h).wait_recv()

                matmul_piece(row * 2 + jnp.where(side, 1 - y, y))
            return carry

        lax.fori_loop(0, 5, piece_step, 0)
        return carry

    lax.fori_loop(1, rows + 2, gather, 0)

    o_own = pltpu.make_async_copy(og.at[:, span(d, block)], xout.at[d], o_sem)
    o_own.start()
    o_other = remote(og.at[:, span(partner, block)], xout.at[d], o_send, o_recv, partner, t)
    o_other.start()

    def late(j, carry):
        f = span(j, size)
        grad = acc[:, f]
        both_all[d, :, span(2 * j, size)] = (grad * slopes_up[:, f]).astype(jnp.bfloat16)
        both_all[d, :, span(2 * j + 1, size)] = (grad * silu[:, f].astype(jnp.float32)).astype(jnp.bfloat16)
        send_own(1, j)
        return carry

    lax.fori_loop(0, LATE, late, 0)

    steps = max(n_in + 2 * (rows - 2), n_out + LAG + 2 * (rows - 1))

    def wave(s, carry):
        wave_step(s)
        return carry

    lax.fori_loop(2, steps, wave, 0)

    def hidden_relay(j, carry):
        relay(0, j)
        return carry

    lax.fori_loop(0, EARLY, hidden_relay, 0)

    def late_relay(j, carry):
        relay(1, j)
        return carry

    lax.fori_loop(0, AHEAD, late_relay, 0)

    def side_wait(i, base, ref):
        @pl.when(has_side)
        def _():
            piece = ref(i, side_col)
            remote(piece, piece, cy_send.at[base + i], cy_recv.at[base + i], d, y_peer).wait_recv()

    def out_side(i, carry):
        side_wait(i, n_in, out_ref)
        return carry

    def in_side(i, carry):
        side_wait(i, 0, in_ref)
        return carry

    lax.fori_loop(0, n_out, out_side, 0)
    o_own.wait()
    o_other.wait()

    def from_partner(a):
        def step(j, carry):
            for r in range(chips):
                core_wait(a, j, r).wait_recv()
            return carry
        return step

    lax.fori_loop(0, EARLY, from_partner(0), 0)

    def product(left, right):
        return jnp.dot(left, right, preferred_element_type=jnp.float32).astype(jnp.bfloat16)

    def down_step(j, carry):
        f = span(j, fw)
        down[f, :] = product(hid_all[:, :, f].reshape(total, fw).T, xout[...].reshape(total, block))
        return carry

    lax.fori_loop(0, hidden // fw, down_step, 0)
    lax.fori_loop(0, n_in, in_side, 0)
    turned[...] = xin[...].reshape(total, block).T

    def main_step(j, carry):
        @pl.when(j >= AHEAD)
        def _():
            relay(1, j)

        @pl.when(j > 0)
        def _():
            from_partner(1)(j - 1, 0)
            f = span(j - 1, size)
            result = product(turned[...], both_all[:, :, f_part(1, j - 1)].reshape(total, 2 * size))
            gate_main[:, f] = result[:, :size]
            up_main[:, f] = result[:, size:]
        return carry

    lax.fori_loop(0, LATE - TAIL + 1, main_step, 0)
    for j in range(LATE - TAIL + 1, LATE):
        relay(1, j)

    def gather_end(s, carry):
        for h in range(SPLIT):
            @pl.when(jnp.logical_and(has_up, z >= s - 1))
            def _():
                up_copy(s, h).wait_send()

            @pl.when(jnp.logical_and(has_down, z + s - 1 < rows))
            def _():
                down_copy(s, h).wait_send()

            across(s - 1, h).wait_send()
        return carry

    lax.fori_loop(1, rows + 1, gather_end, 0)

    @pl.when(jnp.logical_not(owned))
    def _():
        for h in range(SPLIT):
            li_remote(h).wait_send()

    @pl.when(crosses)
    def _():
        for h in range(SPLIT):
            og_far(h).wait_send()

    def chain_end(i, base, ref, head):
        up_next, down_next, side = chain(i, base, ref)
        go_up, go_down = goes(head)

        @pl.when(go_up)
        def _():
            up_next.wait_send()

        @pl.when(go_down)
        def _():
            down_next.wait_send()

        @pl.when(in_chain)
        def _():
            side.wait_send()

    def in_end(i, carry):
        chain_end(i, 0, in_ref, in_head)
        return carry

    def out_end(i, carry):
        chain_end(i, n_in, out_ref, out_head)
        return carry

    lax.fori_loop(0, n_in, in_end, 0)
    lax.fori_loop(0, n_out, out_end, 0)

    def sent(a):
        def step(j, carry):
            own_core(a, j).wait_send()
            for r in range(1, chips):
                own_chip(a, j, r).wait_send()
                pass_core(a, j, r).wait_send()
            return carry
        return step

    for a in range(2):
        lax.fori_loop(0, pieces[a], sent(a), 0)
    lax.fori_loop(LATE - TAIL, LATE, from_partner(1), 0)


def finish(down_in, gate_in, up_in, turned, both_all, down_out, gate_out, up_out, gate_tail, up_tail, sems):
    n_dp, tokens, hidden2 = both_all.shape
    total = n_dp * tokens
    main = gate_in.shape[1]
    size = hidden2 // 2 // LATE
    copies = [
        pltpu.make_async_copy(down_in, down_out, sems.at[0]),
        pltpu.make_async_copy(gate_in, gate_out.at[:, :main], sems.at[1]),
        pltpu.make_async_copy(up_in, up_out.at[:, :main], sems.at[2]),
    ]
    for copy in copies:
        copy.start()
    for j in range(TAIL):
        f = slice(main + j * size, main + (j + 1) * size)
        acts = both_all[:, :, 2 * f.start:2 * f.stop].reshape(total, 2 * size)
        result = jnp.dot(turned[...], acts, preferred_element_type=jnp.float32).astype(jnp.bfloat16)
        gate_tail[j] = result[:, :size]
        up_tail[j] = result[:, size:]
        for k, (tail, out) in enumerate(((gate_tail, gate_out), (up_tail, up_out))):
            copies.append(pltpu.make_async_copy(tail.at[j], out.at[:, f], sems.at[3 + j * 2 + k]))
            copies[-1].start()
    for copy in copies:
        copy.wait()


def shards(n_dp, n_t, out_grad, layer_input, w_down, silu_gate, up_proj, slope_codes):
    hidden, width = w_down.shape
    cols = out_grad.shape[2]
    tokens = out_grad.shape[0] * out_grad.shape[1]
    chips, rows, block = n_dp // 2, n_t // 2, width // n_dp
    words = tokens // 10
    total = n_dp * tokens
    row, col = np.arange(tokens)[:, None], np.arange(tokens)[None, :]
    spread = jnp.asarray(col == (row % 10) * words + row // 10, jnp.bfloat16)
    units = (2 * n_dp - 2) * SPLIT
    far = chips - 1
    bf16 = jnp.bfloat16
    dma = pltpu.SemaphoreType.DMA
    vmem = pl.BlockSpec(memory_space=pltpu.VMEM)
    anywhere = pl.BlockSpec(memory_space=pl.ANY)
    main = hidden // LATE * (LATE - TAIL)
    flops = 2 * tokens * hidden * width + 5 * total * hidden * block
    held = pl.pallas_call(
        functools.partial(exchange, n_dp, n_t),
        out_shape=tuple(pltpu.VMEM(shape, bf16) for shape in (
            (hidden, block), (block, main), (block, main), (block, total),
            (n_dp, tokens, 2 * hidden))),
        in_specs=[anywhere] * 7,
        out_specs=[vmem] * 5,
        scratch_shapes=[
            pltpu.VMEM((tokens, width), bf16),
            pltpu.VMEM((tokens, cols), bf16),
            pltpu.VMEM((tokens, hidden), bf16),
            pltpu.VMEM((tokens, hidden), bf16),
            pltpu.VMEM((words, hidden), jnp.int32),
            pltpu.VMEM((tokens, tokens), bf16),
            pltpu.VMEM((hidden, width), bf16),
            pltpu.VMEM((tokens, hidden), jnp.float32),
            pltpu.VMEM((tokens, hidden), jnp.float32),
            pltpu.VMEM((n_dp, tokens, hidden), bf16),
            pltpu.VMEM((n_dp, tokens, block), bf16),
            pltpu.VMEM((n_dp, tokens, block), bf16),
            dma((6,)), dma((max(1, hidden // min(512, hidden)),)),
            dma((rows + 2, SPLIT)), dma((rows + 2, SPLIT)), dma((rows + 2, SPLIT)), dma((rows + 2, SPLIT)),
            dma((rows, SPLIT)), dma((rows, SPLIT)),
            dma((2 * SPLIT,)), dma((units,)), dma((units,)), dma((units,)), dma((units,)), dma((units,)),
            dma, dma, dma,
            dma((2, far, LATE)), dma((2, far, LATE)), dma((2, chips, LATE)), dma((2, chips, LATE)),
        ],
        compiler_params=pltpu.CompilerParams(
            collective_id=0, has_side_effects=True, vmem_limit_bytes=38 * 1024 * 1024),
        cost_estimate=pl.CostEstimate(flops=flops, bytes_accessed=20_000_000, transcendentals=0),
    )(
        out_grad.reshape(tokens, cols), layer_input.reshape(tokens, cols),
        silu_gate.reshape(tokens, hidden), up_proj.reshape(tokens, hidden),
        slope_codes.reshape(words, hidden), spread, w_down,
    )
    across = jax.ShapeDtypeStruct((block, hidden), bf16)
    size = hidden // LATE
    return pl.pallas_call(
        finish,
        out_shape=(jax.ShapeDtypeStruct((hidden, block), bf16), across, across),
        in_specs=[vmem] * 5,
        out_specs=[anywhere] * 3,
        scratch_shapes=[
            pltpu.VMEM((TAIL, block, size), bf16), pltpu.VMEM((TAIL, block, size), bf16), dma((3 + 2 * TAIL,))],
        compiler_params=pltpu.CompilerParams(vmem_limit_bytes=12 * 1024 * 1024),
    )(*(pltpu.with_memory_space_constraint(value, pltpu.VMEM) for value in held))


def solution(mesh):
    n_dp, n_t = mesh.shape["dp"], mesh.shape["tensor"]
    return jax.shard_map(
        functools.partial(shards, n_dp, n_t),
        mesh=mesh,
        in_specs=(
            P(None, "dp", "tensor"),
            P(None, "dp", "tensor"),
            P("tensor", None),
            P(None, "dp", "tensor"),
            P(None, "dp", "tensor"),
            P(None, "dp", "tensor"),
        ),
        out_specs=(P("tensor", "dp"), P("dp", "tensor"), P("dp", "tensor")),
        check_vma=False,
    )
```

```python
import functools

import jax
import jax.numpy as jnp
import numpy as np
from jax import lax
from jax.experimental import pallas as pl
from jax.experimental.pallas import tpu as pltpu
from jax.sharding import PartitionSpec as P

SLOPE_LEVELS = (-0.09, 0.06, 0.22, 0.41, 0.6, 0.79, 0.96, 1.08)
MESH = pl.DeviceIdType.MESH
EARLY = 4
HELD = 1
LATE = 8
DOWN_AT = 4
RELAY_AT = 9
THEN = 3
AHEAD = 1
TAIL = 1
OG_SPLIT = 4
SPLIT = 2
IN_PACE = 1
IN_HOP = 3
SIDE_LAG = 2
OUT_PACE = 2
OUT_HOP = 2
WAVE_AT = 0
LAG = 5


def exchange(n_dp, n_t, out_hbm, in_hbm, silu_hbm, up_hbm, code_hbm, spread_hbm, w_hbm,
             down, gate_main, up_main, turned, both_all,
             og, li, silu, up, codes, spread, w, slopes_up, acc, hid_all, xin, xout,
             l_sem, w_sem, u_send, u_recv, d_send, d_recv, y_send, y_recv,
             x_send, c_recv, zu_send, zd_send, cy_send, cy_recv, o_sem, o_send, o_recv,
             ax_send, ac_send, hx_recv, hc_recv, hp_recv, ax_recv, ac_recv, ap_recv):
    chips = n_dp // 2
    rows = n_t // 2
    ratio = n_t // n_dp
    tokens, cols = out_hbm.shape
    hidden, width = w_hbm.shape
    block = width // n_dp
    part = cols // SPLIT
    fine = min(OG_SPLIT, cols // 128)
    total = n_dp * tokens
    n_in, n_out = n_dp * SPLIT, (n_dp - 2) * SPLIT
    n_all = n_out * ratio
    acts = (hid_all, both_all)
    pieces = (EARLY, LATE)
    size = hidden // LATE

    d = lax.axis_index("dp")
    t = lax.axis_index("tensor")
    q, c = d // 2, lax.rem(d, 2)
    z, y = t // 2, lax.rem(t, 2)
    partner = q * 2 + (1 - c)
    y_peer = z * 2 + (1 - y)
    z_up = lax.min(z + 1, rows - 1) * 2 + y
    z_down = lax.max(z - 1, 0) * 2 + y
    has_up, has_down = z + 1 < rows, z > 0
    owner = t // ratio
    if ratio == 2:
        in_chain = d >= 0
        has_side = d >= 0
        chain_col, side_col = y, 1 - y
    else:
        in_chain = lax.rem(d, 2) == y
        has_side = lax.rem(d, 2) != y
        chain_col, side_col = y * 0, y * 0
    in_head = (d * ratio) // 2
    out_head = lax.rem(in_head + rows // 2, rows)

    def chip_at(r):
        return lax.rem(q + r, chips) * 2 + c

    def group_from(r, core):
        return lax.rem(q + chips - r, chips) * 2 + core

    def span(index, size):
        return pl.ds(pl.multiple_of(index * size, 128), size)

    def remote(src, dst, send, recv, dp, tensor):
        return pltpu.make_async_remote_copy(
            src_ref=src, dst_ref=dst, send_sem=send, recv_sem=recv,
            device_id={"dp": dp, "tensor": tensor}, device_id_type=MESH)

    my_cols = og.at[:, span(t, cols)]
    loads = [
        pltpu.make_async_copy(out_hbm, my_cols, l_sem.at[0]),
        pltpu.make_async_copy(in_hbm, li, l_sem.at[1]),
        pltpu.make_async_copy(silu_hbm, silu, l_sem.at[2]),
        pltpu.make_async_copy(up_hbm, up, l_sem.at[3]),
        pltpu.make_async_copy(code_hbm, codes, l_sem.at[4]),
        pltpu.make_async_copy(spread_hbm, spread, l_sem.at[5]),
    ]
    for load in loads:
        load.start()

    fw = min(512, hidden)

    def w_copy(j):
        f = span(j, fw)
        return pltpu.make_async_copy(w_hbm.at[f], w.at[f], w_sem)

    barrier = pltpu.get_barrier_semaphore()
    greet = [(d, y_peer), (partner, t)]
    greet += [(chip_at(r), t) for r in range(1, chips)]
    for r in range(1, chips):
        greet.append((lax.rem(q + r, chips) * 2 + 1 - c, t))
    for dp, tensor in greet:
        pl.semaphore_signal(barrier, inc=1, device_id={"dp": dp, "tensor": tensor}, device_id_type=MESH)

    @pl.when(has_up)
    def _():
        pl.semaphore_signal(barrier, inc=1, device_id={"dp": d, "tensor": z_up}, device_id_type=MESH)

    @pl.when(has_down)
    def _():
        pl.semaphore_signal(barrier, inc=1, device_id={"dp": d, "tensor": z_down}, device_id_type=MESH)

    at_end = jnp.logical_or(z == 0, z == rows - 1)

    pl.semaphore_wait(barrier, len(greet) + has_up.astype(jnp.int32) + has_down.astype(jnp.int32))

    def og_piece(row, col, h):
        return og.at[:, span((row * 2 + col) * fine + h, cols // fine)]

    def up_copy(s, h):
        piece = og_piece(lax.max(z - s + 1, 0), y, h)
        return remote(piece, piece, u_send, u_recv.at[s - 1, h], d, z_up)

    def down_copy(s, h):
        piece = og_piece(lax.min(z + s - 1, rows - 1), y, h)
        return remote(piece, piece, d_send, d_recv.at[s - 1, h], d, z_down)

    def up_wait(s, h):
        piece = og_piece(lax.max(z - s, 0), y, h)
        return remote(piece, piece, u_send, u_recv.at[s - 1, h], d, z_up)

    def down_wait(s, h):
        piece = og_piece(lax.min(z + s, rows - 1), y, h)
        return remote(piece, piece, d_send, d_recv.at[s - 1, h], d, z_down)

    def across(row, h):
        piece = og_piece(row, y, h)
        return remote(piece, piece, y_send, y_recv.at[row], d, y_peer)

    def across_wait(row):
        piece = og.at[:, span(row * 2 + 1 - y, cols)]
        return remote(piece, piece, y_send, y_recv.at[row], d, y_peer)

    loads[0].wait()

    for h in range(fine):
        across(z, h).start()

        @pl.when(has_up)
        def _():
            up_copy(1, h).start()

        @pl.when(has_down)
        def _():
            down_copy(1, h).start()

    def in_piece(group, col, h):
        return xin.at[group, :, span(col * SPLIT + h, part)]

    def out_piece(group, col, h):
        return xout.at[group, :, span(col * SPLIT + h, part)]

    in_slot = (lax.rem(owner // 2 + chips - q, chips) * 2 + c) * SPLIT

    def li_remote(h):
        return remote(li.at[:, h * part:(h + 1) * part], in_piece(d, chain_col_of(t), h),
                      x_send.at[0], c_recv.at[in_slot + h], owner, t)

    def li_local(h):
        return pltpu.make_async_copy(li.at[:, h * part:(h + 1) * part], in_piece(d, chain_col_of(t), h),
                                     c_recv.at[in_slot + h])

    def chain_col_of(tensor):
        return lax.rem(tensor, 2) if ratio == 2 else tensor * 0

    loads[1].wait()
    owned = owner == d

    @pl.when(owned)
    def _():
        for h in range(SPLIT):
            li_local(h).start()

    @pl.when(jnp.logical_not(owned))
    def _():
        for h in range(SPLIT):
            li_remote(h).start()

    far_row = lax.rem(z + rows // 2, rows)
    far_owner = (far_row * 2 + y) // ratio
    crosses = far_owner // 2 != q
    far_dist = lax.max(lax.rem(far_owner // 2 + chips - q, chips), 1)
    out_slot = n_in + ((far_dist - 1) * 2 + c) * SPLIT

    def og_far(h):
        src = og.at[:, span((far_row * 2 + y) * SPLIT + h, part)]
        return remote(src, out_piece(d, chain_col_of(t), h),
                      x_send.at[1], c_recv.at[out_slot + h], far_owner, t)

    def f_part(a, j):
        return span(j, acts[a].shape[2] // pieces[a])

    def own_chip(a, j, r):
        own = acts[a].at[d, :, f_part(a, j)]
        land = hx_recv.at[r - 1] if a == 0 else ax_recv.at[r - 1, j]
        return remote(own, own, ax_send.at[a, r - 1], land, chip_at(r), t)

    def own_core(a, j):
        own = acts[a].at[d, :, f_part(a, j)]
        return remote(own, own, ac_send.at[a, 0], (ac_recv if a else hc_recv), partner, t)

    def send_own(a, j):
        for r in range(1, chips):
            own_chip(a, j, r).start()
        own_core(a, j).start()

    def chip_hidden(r):
        land = hid_all.at[group_from(r, c)]
        return remote(land, land, ac_send.at[0, r], hx_recv.at[r - 1], partner, t)

    def pass_hidden(r, core):
        land = hid_all.at[group_from(r, core)]
        return remote(land, land, ac_send.at[0, r], hp_recv.at[r - 1], partner, t)

    def chip_late(j, r):
        land = both_all.at[group_from(r, c), :, f_part(1, j)]
        return remote(land, land, ac_send.at[1, r], ax_recv.at[r - 1, j], partner, t)

    def pass_late(j, r, core):
        land = both_all.at[group_from(r, core), :, f_part(1, j)]
        return remote(land, land, ac_send.at[1, r], ap_recv.at[r - 1, j], partner, t)

    def relay(j):
        for r in range(1, chips):
            chip_late(j, r).wait_recv()
            pass_late(j, r, c).start()

    def arrived(j):
        for r in range(1, chips):
            pass_late(j, r, 1 - c).wait_recv()

    loads[2].wait()
    loads[3].wait()
    for j in range(hidden // fw):
        w_copy(j).start()

    def early(j, carry):
        f = f_part(0, j)
        hid_all[d, :, f] = (silu[:, f].astype(jnp.float32) * up[:, f].astype(jnp.float32)).astype(jnp.bfloat16)

        @pl.when(j < EARLY - HELD)
        def _():
            send_own(0, j)
        return carry

    lax.fori_loop(0, EARLY, early, 0)

    loads[4].wait()
    loads[5].wait()
    acc[...] = jnp.zeros_like(acc)

    def decode(j, carry):
        f = span(j, fw)
        words = codes[:, f]
        symbols = jnp.dot(
            spread[...],
            jnp.concatenate([((words >> (3 * k)) & 7).astype(jnp.float32).astype(jnp.bfloat16) for k in range(10)], axis=0),
            preferred_element_type=jnp.float32)
        slopes = jnp.full(symbols.shape, SLOPE_LEVELS[0], jnp.float32)
        for s in range(1, 8):
            slopes = jnp.where(symbols > s - 0.5, jnp.float32(SLOPE_LEVELS[s]), slopes)
        slopes_up[:, f] = up[:, f].astype(jnp.float32) * slopes
        return carry

    lax.fori_loop(0, hidden // fw, decode, 0)

    def unit(i):
        h, u = lax.rem(i, SPLIT), i // SPLIT
        return lax.rem(u, 2), u // 2, h

    def in_ref(i, col):
        core, r, h = unit(i)
        return in_piece(group_from(r, core), col, h)

    def in_copies(i):
        piece = in_ref(i, chain_col)
        return (remote(piece, piece, zu_send.at[0], c_recv.at[i], d, z_up),
                remote(piece, piece, zd_send.at[0], c_recv.at[i], d, z_down),
                remote(piece, piece, cy_send.at[0], cy_recv, d, y_peer))

    in_up = jnp.logical_and(in_chain, jnp.logical_and(z >= in_head, has_up))
    in_down = jnp.logical_and(in_chain, jnp.logical_and(z <= in_head, has_down))

    def in_rows(i):
        up_next, down_next, side = in_copies(i)
        up_next.wait_recv()

        @pl.when(in_up)
        def _():
            up_next.start()

        @pl.when(in_down)
        def _():
            down_next.start()

    def head_wait(i, carry):
        in_copies(i)[0].wait_recv()
        return carry

    def head_up(i, carry):
        in_copies(i)[0].start()
        return carry

    def head_down(i, carry):
        in_copies(i)[1].start()
        return carry

    def in_side(i, carry):
        in_copies(i)[2].start()
        return carry

    out_up = jnp.logical_and(z >= out_head, has_up)
    out_down = jnp.logical_and(z <= out_head, has_down)
    at_out_head = z == out_head

    in_far = lax.max(z - in_head, in_head - z)
    out_far = lax.max(z - out_head, out_head - z)
    out_last = jnp.logical_and(at_end, out_far > jnp.where(in_chain, in_far, 0))

    def out_step(i):
        if ratio == 2:
            native, other = i < n_out, i + n_out
            col = jnp.where(native, y, 1 - y)
        else:
            native, other, col = in_chain, i, y * 0
        core, r, h = unit(lax.rem(i, n_out))
        piece = out_piece(group_from(r + 1, core), col, h)
        n = n_in + i
        up_next = remote(piece, piece, zu_send.at[1], c_recv.at[n], d, z_up)
        down_next = remote(piece, piece, zd_send.at[1], c_recv.at[n], d, z_down)
        side = remote(piece, piece, cy_send.at[1], c_recv.at[n_in + lax.min(other, n_all - 1)], d, y_peer)
        up_next.wait_recv()

        @pl.when(jnp.logical_and(native, at_out_head))
        def _():
            side.start()

        @pl.when(out_up)
        def _():
            up_next.start()

        @pl.when(out_down)
        def _():
            down_next.start()

    at_in_head = jnp.logical_and(in_chain, in_far == 0)

    def matmul_piece(piece):
        k = span(piece, cols)
        acc[...] += lax.dot_general(og[:, k], w[:, k], (((1,), (1,)), ((), ())),
                                    preferred_element_type=jnp.float32)

    def wave_step(s):
        past = jnp.logical_and(in_chain, in_far > 0)
        first = IN_PACE * (s - IN_HOP * (in_far - 1))
        for i in range(IN_PACE):
            @pl.when(jnp.logical_and(past, jnp.logical_and(first + i >= 0, first + i < n_in)))
            def _():
                in_rows(first + i)

        late_side = first - IN_PACE * SIDE_LAG
        for i in range(IN_PACE):
            @pl.when(jnp.logical_and(past, jnp.logical_and(late_side + i >= 0, late_side + i < n_in)))
            def _():
                in_side(late_side + i, 0)

        out_first = OUT_PACE * (s - LAG - OUT_HOP * out_far)
        for i in range(OUT_PACE):
            @pl.when(jnp.logical_and(jnp.logical_not(out_last), jnp.logical_and(out_first + i >= 0, out_first + i < n_all)))
            def _():
                out_step(out_first + i)

    order, place = [], 0
    for dist in range(rows + 1):
        for far_side in (0, 1):
            away = dist - far_side
            for way in ((-1, 1) if away > 0 else (1,) if away == 0 else ()):
                row = z + way * away
                valid = jnp.logical_and(row >= 0, row < rows)
                order.append((valid, place, row, far_side))
                place = place + valid.astype(jnp.int32)

    def multiply(p):
        row, side = 0, 0
        for valid, place, its_row, far_side in order:
            mine = jnp.logical_and(valid, place == p)
            row = jnp.where(mine, its_row, row)
            side = jnp.where(mine, far_side, side)

        @pl.when(side == 1)
        def _():
            across_wait(row).wait_recv()

        matmul_piece(row * 2 + jnp.where(side == 1, 1 - y, y))

    arrivals = fine * (rows - 1)

    def gather(e, carry):
        s, h = e // fine + 1, lax.rem(e, fine)
        last_part = h == fine - 1

        @pl.when(z >= s)
        def _():
            up_wait(s, h).wait_recv()

            @pl.when(has_up)
            def _():
                up_copy(s + 1, h).start()

            across(lax.max(z - s, 0), h).start()

        @pl.when(z + s < rows)
        def _():
            down_wait(s, h).wait_recv()

            @pl.when(has_down)
            def _():
                down_copy(s + 1, h).start()

            across(lax.min(z + s, rows - 1), h).start()

        @pl.when(jnp.logical_and(s == rows // 2, last_part))
        def _():
            @pl.when(crosses)
            def _():
                for k in range(SPLIT):
                    og_far(k).start()

            for j in range(EARLY - HELD, EARLY):
                send_own(0, j)

        @pl.when(jnp.logical_and(last_part, at_in_head))
        def _():
            @pl.when(s == 1)
            def _():
                lax.fori_loop(near, n_in, head_wait, 0)

            @pl.when(jnp.logical_and(in_up, s == lax.max(z, 1)))
            def _():
                lax.fori_loop(jnp.where(z == 0, near, 0), n_in, head_up, 0)

            @pl.when(jnp.logical_and(in_down, s == lax.max(rows - 1 - z, 1)))
            def _():
                lax.fori_loop(jnp.where(z == rows - 1, near, 0), n_in, head_down, 0)

        @pl.when(jnp.logical_and(jnp.logical_and(s == rows - 1, last_part), at_in_head))
        def _():
            lax.fori_loop(0, n_in, in_side, 0)

        @pl.when(e == fine - 1)
        def _():
            pltpu.make_async_copy(w_hbm, w, w_sem).wait()

        pace = max(fine // 2, 1)
        p = jnp.where(e < arrivals, (e + 1) // pace - 2, e - arrivals + arrivals // pace - 1)
        now = jnp.logical_and(p >= 0, jnp.logical_or(e >= arrivals, lax.rem(e + 1, pace) == 0))

        @pl.when(jnp.logical_and(now, p >= 3 + WAVE_AT))
        def _():
            wave_step(p - 3 - WAVE_AT)

        @pl.when(now)
        def _():
            multiply(p)
        return carry

    near = 2 * SPLIT

    @pl.when(at_in_head)
    def _():
        lax.fori_loop(0, near, head_wait, 0)

        @pl.when(z == 0)
        def _():
            lax.fori_loop(0, near, head_up, 0)

        @pl.when(z == rows - 1)
        def _():
            lax.fori_loop(0, near, head_down, 0)

    lax.fori_loop(0, arrivals + n_t - arrivals // max(fine // 2, 1) + 1, gather, 0)

    o_own = pltpu.make_async_copy(og.at[:, span(d, block)], xout.at[d], o_sem)
    o_own.start()
    o_other = remote(og.at[:, span(partner, block)], xout.at[d], o_send, o_recv, partner, t)
    o_other.start()

    def late(j, carry):
        f = span(j, size)
        grad = acc[:, f]
        both_all[d, :, span(2 * j, size)] = (grad * slopes_up[:, f]).astype(jnp.bfloat16)
        both_all[d, :, span(2 * j + 1, size)] = (grad * silu[:, f].astype(jnp.float32)).astype(jnp.bfloat16)
        send_own(1, j)
        return carry

    lax.fori_loop(0, LATE, late, 0)

    steps = max(-(-n_in // IN_PACE) + SIDE_LAG + IN_HOP * (rows - 2), -(-n_all // OUT_PACE) + LAG + OUT_HOP * (rows - 1))

    def wave(s, carry):
        @pl.when(s == RELAY_AT)
        def _():
            for r in range(1, chips):
                chip_hidden(r).wait_recv()
                pass_hidden(r, c).start()

        wave_step(s)
        return carry

    lax.fori_loop(n_t - 3 - WAVE_AT, steps, wave, 0)

    def late_relay(j, carry):
        relay(j)
        return carry

    lax.fori_loop(0, AHEAD, late_relay, 0)

    def product(left, right):
        return jnp.dot(left, right, preferred_element_type=jnp.float32).astype(jnp.bfloat16)

    def down_product():
        o_own.wait()
        o_other.wait()
        theirs = hid_all.at[partner]
        remote(theirs, theirs, ac_send.at[0, 0], hc_recv, partner, t).wait_recv()
        for r in range(1, chips):
            pass_hidden(r, 1 - c).wait_recv()

        def down_step(j, carry):
            f = span(j, fw)
            down[f, :] = product(hid_all[:, :, f].reshape(total, fw).T, xout[...].reshape(total, block))
            return carry

        lax.fori_loop(0, hidden // fw, down_step, 0)

    @pl.when(jnp.logical_not(out_last))
    def _():
        down_product()

    lax.fori_loop(AHEAD, THEN, late_relay, 0)
    columns = xin.at[:, :, :cols]

    @pl.when(has_side)
    def _():
        remote(columns, columns, cy_send.at[0], cy_recv, d, y_peer).wait_recv()

    turned[...] = xin[...].reshape(total, block).T
    theirs_late = both_all.at[partner]
    remote(theirs_late, theirs_late, ac_send.at[1, 0], ac_recv, partner, t).wait_recv()

    def main_step(j, carry):
        @pl.when(j >= THEN)
        def _():
            relay(j)

        @pl.when(j > 0)
        def _():
            arrived(j - 1)
            f = span(j - 1, size)
            result = product(turned[...], both_all[:, :, f_part(1, j - 1)].reshape(total, 2 * size))
            gate_main[:, f] = result[:, :size]
            up_main[:, f] = result[:, size:]
        return carry

    lax.fori_loop(0, DOWN_AT, main_step, 0)

    @pl.when(out_last)
    def _():
        def take(i, carry):
            out_step(i)
            return carry

        lax.fori_loop(0, n_all, take, 0)
        down_product()

    lax.fori_loop(DOWN_AT, LATE - TAIL + 1, main_step, 0)

    def sent(ref, sem):
        remote(ref, ref, sem, c_recv.at[0], partner, t).wait_send()

    for k in range(rows):
        ups = k + 1
        downs = rows - k

        @pl.when(jnp.logical_and(z == k, has_up))
        def _():
            sent(og.at[:, :ups * cols], u_send)

        @pl.when(jnp.logical_and(z == k, has_down))
        def _():
            sent(og.at[:, :downs * cols], d_send)

    sent(og.at[:, :rows * cols], y_send)

    @pl.when(jnp.logical_not(owned))
    def _():
        sent(li, x_send.at[0])

    @pl.when(crosses)
    def _():
        sent(li, x_send.at[1])

    far_out = xout.at[:n_dp - 2]
    for flag, ref, sem in (
            (in_up, columns, zu_send.at[0]), (in_down, columns, zd_send.at[0]), (in_chain, columns, cy_send.at[0]),
            (out_up, far_out, zu_send.at[1]), (out_down, far_out, zd_send.at[1]),
            (jnp.logical_and(in_chain, at_out_head), xout.at[:n_dp - 2, :, :cols], cy_send.at[1])):
        @pl.when(flag)
        def _():
            sent(ref, sem)

    for a in range(2):
        own = acts[a].at[d]
        sent(own, ac_send.at[a, 0])
        for r in range(1, chips):
            sent(own, ax_send.at[a, r - 1])
            if a == 0:
                sent(own, ac_send.at[0, r])
    for j in range(LATE - TAIL + 1, LATE):
        relay(j)
    for j in range(LATE - TAIL, LATE):
        arrived(j)
    for r in range(1, chips):
        sent(both_all.at[d], ac_send.at[1, r])


def finish(down_in, gate_in, up_in, turned, both_all, down_out, gate_out, up_out, gate_tail, up_tail, sems):
    n_dp, tokens, hidden2 = both_all.shape
    total = n_dp * tokens
    main = gate_in.shape[1]
    size = hidden2 // 2 // LATE
    copies = [
        pltpu.make_async_copy(down_in, down_out, sems.at[0]),
        pltpu.make_async_copy(gate_in, gate_out.at[:, :main], sems.at[1]),
        pltpu.make_async_copy(up_in, up_out.at[:, :main], sems.at[2]),
    ]
    for copy in copies:
        copy.start()
    for j in range(TAIL):
        f = slice(main + j * size, main + (j + 1) * size)
        acts = both_all[:, :, 2 * f.start:2 * f.stop].reshape(total, 2 * size)
        result = jnp.dot(turned[...], acts, preferred_element_type=jnp.float32).astype(jnp.bfloat16)
        gate_tail[j] = result[:, :size]
        up_tail[j] = result[:, size:]
        for k, (tail, out) in enumerate(((gate_tail, gate_out), (up_tail, up_out))):
            copies.append(pltpu.make_async_copy(tail.at[j], out.at[:, f], sems.at[3 + j * 2 + k]))
            copies[-1].start()
    for copy in copies:
        copy.wait()


def shards(n_dp, n_t, out_grad, layer_input, w_down, silu_gate, up_proj, slope_codes):
    hidden, width = w_down.shape
    cols = out_grad.shape[2]
    tokens = out_grad.shape[0] * out_grad.shape[1]
    chips, rows, block = n_dp // 2, n_t // 2, width // n_dp
    words = tokens // 10
    total = n_dp * tokens
    row, col = np.arange(tokens)[:, None], np.arange(tokens)[None, :]
    spread = jnp.asarray(col == (row % 10) * words + row // 10, jnp.bfloat16)
    units = (n_dp + (n_dp - 2) * (n_t // n_dp)) * SPLIT
    far = chips - 1
    bf16 = jnp.bfloat16
    dma = pltpu.SemaphoreType.DMA
    vmem = pl.BlockSpec(memory_space=pltpu.VMEM)
    anywhere = pl.BlockSpec(memory_space=pl.ANY)
    main = hidden // LATE * (LATE - TAIL)
    flops = 2 * tokens * hidden * width + 5 * total * hidden * block
    held = pl.pallas_call(
        functools.partial(exchange, n_dp, n_t),
        out_shape=tuple(pltpu.VMEM(shape, bf16) for shape in (
            (hidden, block), (block, main), (block, main), (block, total),
            (n_dp, tokens, 2 * hidden))),
        in_specs=[anywhere] * 7,
        out_specs=[vmem] * 5,
        scratch_shapes=[
            pltpu.VMEM((tokens, width), bf16),
            pltpu.VMEM((tokens, cols), bf16),
            pltpu.VMEM((tokens, hidden), bf16),
            pltpu.VMEM((tokens, hidden), bf16),
            pltpu.VMEM((words, hidden), jnp.int32),
            pltpu.VMEM((tokens, tokens), bf16),
            pltpu.VMEM((hidden, width), bf16),
            pltpu.VMEM((tokens, hidden), jnp.float32),
            pltpu.VMEM((tokens, hidden), jnp.float32),
            pltpu.VMEM((n_dp, tokens, hidden), bf16),
            pltpu.VMEM((n_dp, tokens, block), bf16),
            pltpu.VMEM((n_dp, tokens, block), bf16),
            dma((6,)), dma, dma, dma((rows, OG_SPLIT)), dma, dma((rows, OG_SPLIT)), dma, dma((rows,)),
            dma((2,)), dma((units,)), dma((2,)), dma((2,)), dma((2,)), dma, dma, dma, dma,
            dma((2, far)), dma((2, chips)), dma((far,)), dma, dma((far,)), dma((far, LATE)), dma, dma((far, LATE)),
        ],
        compiler_params=pltpu.CompilerParams(
            collective_id=0, has_side_effects=True, vmem_limit_bytes=38 * 1024 * 1024),
        cost_estimate=pl.CostEstimate(flops=flops, bytes_accessed=20_000_000, transcendentals=0),
    )(
        out_grad.reshape(tokens, cols), layer_input.reshape(tokens, cols),
        silu_gate.reshape(tokens, hidden), up_proj.reshape(tokens, hidden),
        slope_codes.reshape(words, hidden), spread, w_down,
    )
    across = jax.ShapeDtypeStruct((block, hidden), bf16)
    size = hidden // LATE
    return pl.pallas_call(
        finish,
        out_shape=(jax.ShapeDtypeStruct((hidden, block), bf16), across, across),
        in_specs=[vmem] * 5,
        out_specs=[anywhere] * 3,
        scratch_shapes=[
            pltpu.VMEM((TAIL, block, size), bf16), pltpu.VMEM((TAIL, block, size), bf16), dma((3 + 2 * TAIL,))],
        compiler_params=pltpu.CompilerParams(vmem_limit_bytes=12 * 1024 * 1024),
    )(*(pltpu.with_memory_space_constraint(value, pltpu.VMEM) for value in held))


def solution(mesh):
    n_dp, n_t = mesh.shape["dp"], mesh.shape["tensor"]
    return jax.shard_map(
        functools.partial(shards, n_dp, n_t),
        mesh=mesh,
        in_specs=(
            P(None, "dp", "tensor"),
            P(None, "dp", "tensor"),
            P("tensor", None),
            P(None, "dp", "tensor"),
            P(None, "dp", "tensor"),
            P(None, "dp", "tensor"),
        ),
        out_specs=(P("tensor", "dp"), P("dp", "tensor"), P("dp", "tensor")),
        check_vma=False,
    )
```

```python
import functools

import jax
import jax.numpy as jnp
import numpy as np
from jax import lax
from jax.experimental import pallas as pl
from jax.experimental.pallas import tpu as pltpu
from jax.sharding import PartitionSpec as P

SLOPE_LEVELS = (-0.09, 0.06, 0.22, 0.41, 0.6, 0.79, 0.96, 1.08)
MESH = pl.DeviceIdType.MESH
EARLY = 4
HELD = 1
LATE = 8
DOWN_AT = 5
RELAY_AT = 9
THEN = 3
AHEAD = 1
TAIL = 1
OG_SPLIT = 4
SPLIT = 2
IN_PACE = 1
IN_HOP = 3
SIDE_LAG = 2
OUT_PACE = 2
OUT_HOP = 2
WAVE_AT = 0
LAG = 5


def exchange(n_dp, n_t, out_hbm, in_hbm, silu_hbm, up_hbm, code_hbm, spread_hbm, w_hbm,
             down, gate_main, up_main, turned, both_all,
             og, li, silu, up, codes, spread, w, slopes_up, acc, hid_all, xin, xout,
             l_sem, w_sem, u_send, d_send, r_recv, y_send, y_recv,
             x_send, c_recv, zu_send, zd_send, cy_send, cy_recv, o_sem, o_send, o_recv,
             ax_send, ac_send, hx_recv, hc_recv, hp_recv, ax_recv, ac_recv, ap_recv):
    chips = n_dp // 2
    rows = n_t // 2
    ratio = n_t // n_dp
    tokens, cols = out_hbm.shape
    hidden, width = w_hbm.shape
    block = width // n_dp
    part = cols // SPLIT
    fine = min(OG_SPLIT, cols // 128)
    total = n_dp * tokens
    n_in, n_out = n_dp * SPLIT, (n_dp - 2) * SPLIT
    n_all = n_out * ratio
    acts = (hid_all, both_all)
    pieces = (EARLY, LATE)
    size = hidden // LATE

    d = lax.axis_index("dp")
    t = lax.axis_index("tensor")
    q, c = d // 2, lax.rem(d, 2)
    z, y = t // 2, lax.rem(t, 2)
    partner = q * 2 + (1 - c)
    y_peer = z * 2 + (1 - y)
    z_up = lax.min(z + 1, rows - 1) * 2 + y
    z_down = lax.max(z - 1, 0) * 2 + y
    has_up, has_down = z + 1 < rows, z > 0
    owner = t // ratio
    if ratio == 2:
        in_chain = d >= 0
        has_side = d >= 0
        chain_col, side_col = y, 1 - y
    else:
        in_chain = lax.rem(d, 2) == y
        has_side = lax.rem(d, 2) != y
        chain_col, side_col = y * 0, y * 0
    in_head = (d * ratio) // 2
    out_head = lax.rem(in_head + rows // 2, rows)

    def chip_at(r):
        return lax.rem(q + r, chips) * 2 + c

    def group_from(r, core):
        return lax.rem(q + chips - r, chips) * 2 + core

    def span(index, size):
        return pl.ds(pl.multiple_of(index * size, 128), size)

    def remote(src, dst, send, recv, dp, tensor):
        return pltpu.make_async_remote_copy(
            src_ref=src, dst_ref=dst, send_sem=send, recv_sem=recv,
            device_id={"dp": dp, "tensor": tensor}, device_id_type=MESH)

    my_cols = og.at[:, span(t, cols)]
    loads = [
        pltpu.make_async_copy(out_hbm, my_cols, l_sem.at[0]),
        pltpu.make_async_copy(in_hbm, li, l_sem.at[1]),
        pltpu.make_async_copy(silu_hbm, silu, l_sem.at[2]),
        pltpu.make_async_copy(up_hbm, up, l_sem.at[3]),
        pltpu.make_async_copy(code_hbm, codes, l_sem.at[4]),
        pltpu.make_async_copy(spread_hbm, spread, l_sem.at[5]),
    ]
    for load in loads:
        load.start()

    fw = min(512, hidden)

    def w_copy(j):
        f = span(j, fw)
        return pltpu.make_async_copy(w_hbm.at[f], w.at[f], w_sem)

    barrier = pltpu.get_barrier_semaphore()
    greet = [(d, y_peer), (partner, t)]
    greet += [(chip_at(r), t) for r in range(1, chips)]
    for r in range(1, chips):
        greet.append((lax.rem(q + r, chips) * 2 + 1 - c, t))
    for dp, tensor in greet:
        pl.semaphore_signal(barrier, inc=1, device_id={"dp": dp, "tensor": tensor}, device_id_type=MESH)

    @pl.when(has_up)
    def _():
        pl.semaphore_signal(barrier, inc=1, device_id={"dp": d, "tensor": z_up}, device_id_type=MESH)

    @pl.when(has_down)
    def _():
        pl.semaphore_signal(barrier, inc=1, device_id={"dp": d, "tensor": z_down}, device_id_type=MESH)

    at_end = jnp.logical_or(z == 0, z == rows - 1)

    pl.semaphore_wait(barrier, len(greet) + has_up.astype(jnp.int32) + has_down.astype(jnp.int32))

    def og_piece(row, col, h):
        return og.at[:, span((row * 2 + col) * fine + h, cols // fine)]

    def along(row, h, send, tensor):
        piece = og_piece(row, y, h)
        return remote(piece, piece, send, r_recv.at[row, h], d, tensor)

    def up_copy(s, h):
        return along(lax.max(z - s + 1, 0), h, u_send, z_up)

    def down_copy(s, h):
        return along(lax.min(z + s - 1, rows - 1), h, d_send, z_down)

    def up_wait(s, h):
        return along(lax.max(z - s, 0), h, u_send, z_up)

    def down_wait(s, h):
        return along(lax.min(z + s, rows - 1), h, d_send, z_down)

    def across(row, h):
        piece = og_piece(row, y, h)
        return remote(piece, piece, y_send, y_recv.at[row], d, y_peer)

    def across_wait(row):
        piece = og.at[:, span(row * 2 + 1 - y, cols)]
        return remote(piece, piece, y_send, y_recv.at[row], d, y_peer)

    loads[0].wait()

    for h in range(fine):
        across(z, h).start()

        @pl.when(has_up)
        def _():
            up_copy(1, h).start()

        @pl.when(has_down)
        def _():
            down_copy(1, h).start()

    def in_piece(group, col, h):
        return xin.at[group, :, span(col * SPLIT + h, part)]

    def out_piece(group, col, h):
        return xout.at[group, :, span(col * SPLIT + h, part)]

    in_slot = (lax.rem(owner // 2 + chips - q, chips) * 2 + c) * SPLIT

    def li_remote(h):
        return remote(li.at[:, h * part:(h + 1) * part], in_piece(d, chain_col_of(t), h),
                      x_send.at[0], c_recv.at[in_slot + h], owner, t)

    def li_local(h):
        return pltpu.make_async_copy(li.at[:, h * part:(h + 1) * part], in_piece(d, chain_col_of(t), h),
                                     c_recv.at[in_slot + h])

    def chain_col_of(tensor):
        return lax.rem(tensor, 2) if ratio == 2 else tensor * 0

    loads[1].wait()
    owned = owner == d

    @pl.when(owned)
    def _():
        for h in range(SPLIT):
            li_local(h).start()

    @pl.when(jnp.logical_not(owned))
    def _():
        for h in range(SPLIT):
            li_remote(h).start()

    far_row = lax.rem(z + rows // 2, rows)
    far_owner = (far_row * 2 + y) // ratio
    crosses = far_owner // 2 != q
    far_dist = lax.max(lax.rem(far_owner // 2 + chips - q, chips), 1)
    out_slot = n_in + ((far_dist - 1) * 2 + c) * SPLIT

    def og_far(h):
        src = og.at[:, span((far_row * 2 + y) * SPLIT + h, part)]
        return remote(src, out_piece(d, chain_col_of(t), h),
                      x_send.at[1], c_recv.at[out_slot + h], far_owner, t)

    def f_part(a, j):
        return span(j, acts[a].shape[2] // pieces[a])

    def own_chip(a, j, r):
        own = acts[a].at[d, :, f_part(a, j)]
        land = hx_recv.at[r - 1] if a == 0 else ax_recv.at[r - 1, j]
        return remote(own, own, ax_send.at[a, r - 1], land, chip_at(r), t)

    def own_core(a, j):
        own = acts[a].at[d, :, f_part(a, j)]
        return remote(own, own, ac_send.at[a, 0], (ac_recv if a else hc_recv), partner, t)

    def send_own(a, j):
        for r in range(1, chips):
            own_chip(a, j, r).start()
        own_core(a, j).start()

    def chip_hidden(r):
        land = hid_all.at[group_from(r, c)]
        return remote(land, land, ac_send.at[0, r], hx_recv.at[r - 1], partner, t)

    def pass_hidden(r, core):
        land = hid_all.at[group_from(r, core)]
        return remote(land, land, ac_send.at[0, r], hp_recv.at[r - 1], partner, t)

    def chip_late(j, r):
        land = both_all.at[group_from(r, c), :, f_part(1, j)]
        return remote(land, land, ac_send.at[1, r], ax_recv.at[r - 1, j], partner, t)

    def pass_late(j, r, core):
        land = both_all.at[group_from(r, core), :, f_part(1, j)]
        return remote(land, land, ac_send.at[1, r], ap_recv.at[r - 1, j], partner, t)

    def relay(j):
        for r in range(1, chips):
            chip_late(j, r).wait_recv()
            pass_late(j, r, c).start()

    def arrived(j):
        for r in range(1, chips):
            pass_late(j, r, 1 - c).wait_recv()

    loads[2].wait()
    loads[3].wait()
    for j in range(hidden // fw):
        w_copy(j).start()

    def early(j, carry):
        f = f_part(0, j)
        hid_all[d, :, f] = (silu[:, f].astype(jnp.float32) * up[:, f].astype(jnp.float32)).astype(jnp.bfloat16)

        @pl.when(j < EARLY - HELD)
        def _():
            send_own(0, j)
        return carry

    lax.fori_loop(0, EARLY, early, 0)

    loads[4].wait()
    loads[5].wait()
    acc[...] = jnp.zeros_like(acc)

    def decode(j, carry):
        f = span(j, fw)
        words = codes[:, f]
        symbols = jnp.dot(
            spread[...],
            jnp.concatenate([((words >> (3 * k)) & 7).astype(jnp.float32).astype(jnp.bfloat16) for k in range(10)], axis=0),
            preferred_element_type=jnp.float32)
        slopes = jnp.full(symbols.shape, SLOPE_LEVELS[0], jnp.float32)
        for s in range(1, 8):
            slopes = jnp.where(symbols > s - 0.5, jnp.float32(SLOPE_LEVELS[s]), slopes)
        slopes_up[:, f] = up[:, f].astype(jnp.float32) * slopes
        return carry

    lax.fori_loop(0, hidden // fw, decode, 0)

    def unit(i):
        h, u = lax.rem(i, SPLIT), i // SPLIT
        return lax.rem(u, 2), u // 2, h

    def in_ref(i, col):
        core, r, h = unit(i)
        return in_piece(group_from(r, core), col, h)

    def in_copies(i):
        piece = in_ref(i, chain_col)
        return (remote(piece, piece, zu_send.at[0], c_recv.at[i], d, z_up),
                remote(piece, piece, zd_send.at[0], c_recv.at[i], d, z_down),
                remote(piece, piece, cy_send.at[0], cy_recv, d, y_peer))

    in_up = jnp.logical_and(in_chain, jnp.logical_and(z >= in_head, has_up))
    in_down = jnp.logical_and(in_chain, jnp.logical_and(z <= in_head, has_down))

    def in_rows(i):
        up_next, down_next, side = in_copies(i)
        up_next.wait_recv()

        @pl.when(in_up)
        def _():
            up_next.start()

        @pl.when(in_down)
        def _():
            down_next.start()

    def head_wait(i, carry):
        in_copies(i)[0].wait_recv()
        return carry

    def head_up(i, carry):
        in_copies(i)[0].start()
        return carry

    def head_down(i, carry):
        in_copies(i)[1].start()
        return carry

    def in_side(i, carry):
        in_copies(i)[2].start()
        return carry

    out_up = jnp.logical_and(z >= out_head, has_up)
    out_down = jnp.logical_and(z <= out_head, has_down)
    at_out_head = z == out_head

    in_far = lax.max(z - in_head, in_head - z)
    out_far = lax.max(z - out_head, out_head - z)
    out_last = jnp.logical_and(at_end, out_far > jnp.where(in_chain, in_far, 0))

    def out_step(i):
        if ratio == 2:
            native, other = i < n_out, i + n_out
            col = jnp.where(native, y, 1 - y)
        else:
            native, other, col = in_chain, i, y * 0
        core, r, h = unit(lax.rem(i, n_out))
        piece = out_piece(group_from(r + 1, core), col, h)
        n = n_in + i
        up_next = remote(piece, piece, zu_send.at[1], c_recv.at[n], d, z_up)
        down_next = remote(piece, piece, zd_send.at[1], c_recv.at[n], d, z_down)
        side = remote(piece, piece, cy_send.at[1], c_recv.at[n_in + lax.min(other, n_all - 1)], d, y_peer)
        up_next.wait_recv()

        @pl.when(jnp.logical_and(native, at_out_head))
        def _():
            side.start()

        @pl.when(out_up)
        def _():
            up_next.start()

        @pl.when(out_down)
        def _():
            down_next.start()

    at_in_head = jnp.logical_and(in_chain, in_far == 0)

    def matmul_piece(piece):
        k = span(piece, cols)
        acc[...] += lax.dot_general(og[:, k], w[:, k], (((1,), (1,)), ((), ())),
                                    preferred_element_type=jnp.float32)

    def wave_step(s):
        past = jnp.logical_and(in_chain, in_far > 0)
        first = IN_PACE * (s - IN_HOP * (in_far - 1))
        for i in range(IN_PACE):
            @pl.when(jnp.logical_and(past, jnp.logical_and(first + i >= 0, first + i < n_in)))
            def _():
                in_rows(first + i)

        late_side = first - IN_PACE * SIDE_LAG
        for i in range(IN_PACE):
            @pl.when(jnp.logical_and(past, jnp.logical_and(late_side + i >= 0, late_side + i < n_in)))
            def _():
                in_side(late_side + i, 0)

        out_first = OUT_PACE * (s - LAG - OUT_HOP * out_far)
        for i in range(OUT_PACE):
            @pl.when(jnp.logical_and(jnp.logical_not(out_last), jnp.logical_and(out_first + i >= 0, out_first + i < n_all)))
            def _():
                out_step(out_first + i)

    order, place = [], 0
    for dist in range(rows + 1):
        for far_side in (0, 1):
            away = dist - far_side
            for way in ((-1, 1) if away > 0 else (1,) if away == 0 else ()):
                row = z + way * away
                valid = jnp.logical_and(row >= 0, row < rows)
                order.append((valid, place, row, far_side))
                place = place + valid.astype(jnp.int32)

    def multiply(p):
        row, side = 0, 0
        for valid, place, its_row, far_side in order:
            mine = jnp.logical_and(valid, place == p)
            row = jnp.where(mine, its_row, row)
            side = jnp.where(mine, far_side, side)

        @pl.when(side == 1)
        def _():
            across_wait(row).wait_recv()

        matmul_piece(row * 2 + jnp.where(side == 1, 1 - y, y))

    arrivals = fine * (rows - 1)

    def gather(e, carry):
        s, h = e // fine + 1, lax.rem(e, fine)
        last_part = h == fine - 1

        @pl.when(z >= s)
        def _():
            up_wait(s, h).wait_recv()

            @pl.when(has_up)
            def _():
                up_copy(s + 1, h).start()

            across(lax.max(z - s, 0), h).start()

        @pl.when(z + s < rows)
        def _():
            down_wait(s, h).wait_recv()

            @pl.when(has_down)
            def _():
                down_copy(s + 1, h).start()

            across(lax.min(z + s, rows - 1), h).start()

        @pl.when(jnp.logical_and(s == rows // 2, last_part))
        def _():
            @pl.when(crosses)
            def _():
                for k in range(SPLIT):
                    og_far(k).start()

            for j in range(EARLY - HELD, EARLY):
                send_own(0, j)

        @pl.when(at_in_head)
        def _():
            @pl.when(e == fine - 1)
            def _():
                lax.fori_loop(near, n_in, head_wait, 0)

            @pl.when(jnp.logical_and(in_up, e == fine * lax.max(z, 1) - 1))
            def _():
                lax.fori_loop(jnp.where(z == 0, near, 0), n_in, head_up, 0)

            @pl.when(jnp.logical_and(in_down, e == fine * lax.max(rows - 1 - z, 1) - 1))
            def _():
                lax.fori_loop(jnp.where(z == rows - 1, near, 0), n_in, head_down, 0)

            @pl.when(e == arrivals - 1)
            def _():
                lax.fori_loop(0, n_in, in_side, 0)

        @pl.when(e == fine - 1)
        def _():
            pltpu.make_async_copy(w_hbm, w, w_sem).wait()

        pace = max(fine // 2, 1)
        p = jnp.where(e < arrivals, (e + 1) // pace - 2, e - arrivals + arrivals // pace - 1)
        now = jnp.logical_and(p >= 0, jnp.logical_or(e >= arrivals, lax.rem(e + 1, pace) == 0))

        @pl.when(jnp.logical_and(now, p >= 3 + WAVE_AT))
        def _():
            wave_step(p - 3 - WAVE_AT)

        @pl.when(now)
        def _():
            multiply(p)
        return carry

    near = 2 * SPLIT

    @pl.when(at_in_head)
    def _():
        lax.fori_loop(0, near, head_wait, 0)

        @pl.when(z == 0)
        def _():
            lax.fori_loop(0, near, head_up, 0)

        @pl.when(z == rows - 1)
        def _():
            lax.fori_loop(0, near, head_down, 0)

    lax.fori_loop(0, arrivals + n_t - arrivals // max(fine // 2, 1) + 1, gather, 0)

    o_own = pltpu.make_async_copy(og.at[:, span(d, block)], xout.at[d], o_sem)
    o_own.start()
    o_other = remote(og.at[:, span(partner, block)], xout.at[d], o_send, o_recv, partner, t)
    o_other.start()

    def late(j, carry):
        f = span(j, size)
        grad = acc[:, f]
        both_all[d, :, span(2 * j, size)] = (grad * slopes_up[:, f]).astype(jnp.bfloat16)
        both_all[d, :, span(2 * j + 1, size)] = (grad * silu[:, f].astype(jnp.float32)).astype(jnp.bfloat16)
        send_own(1, j)
        return carry

    lax.fori_loop(0, LATE, late, 0)

    steps = max(-(-n_in // IN_PACE) + SIDE_LAG + IN_HOP * (rows - 2), -(-n_all // OUT_PACE) + LAG + OUT_HOP * (rows - 1))

    def wave(s, carry):
        @pl.when(s == RELAY_AT)
        def _():
            for r in range(1, chips):
                chip_hidden(r).wait_recv()
                pass_hidden(r, c).start()

        wave_step(s)
        return carry

    lax.fori_loop(n_t - 3 - WAVE_AT, steps, wave, 0)

    def late_relay(j, carry):
        relay(j)
        return carry

    lax.fori_loop(0, AHEAD, late_relay, 0)

    def product(left, right):
        return jnp.dot(left, right, preferred_element_type=jnp.float32).astype(jnp.bfloat16)

    def down_product():
        o_own.wait()
        o_other.wait()
        theirs = hid_all.at[partner]
        remote(theirs, theirs, ac_send.at[0, 0], hc_recv, partner, t).wait_recv()
        for r in range(1, chips):
            pass_hidden(r, 1 - c).wait_recv()

        def down_step(j, carry):
            f = span(j, fw)
            down[f, :] = product(hid_all[:, :, f].reshape(total, fw).T, xout[...].reshape(total, block))
            return carry

        lax.fori_loop(0, hidden // fw, down_step, 0)

    @pl.when(jnp.logical_not(out_last))
    def _():
        down_product()

    lax.fori_loop(AHEAD, THEN, late_relay, 0)
    columns = xin.at[:, :, :cols]

    @pl.when(has_side)
    def _():
        remote(columns, columns, cy_send.at[0], cy_recv, d, y_peer).wait_recv()

    turned[...] = xin[...].reshape(total, block).T
    theirs_late = both_all.at[partner]
    remote(theirs_late, theirs_late, ac_send.at[1, 0], ac_recv, partner, t).wait_recv()

    def main_step(j, carry):
        @pl.when(j >= THEN)
        def _():
            relay(j)

        @pl.when(j > 0)
        def _():
            arrived(j - 1)
            f = span(j - 1, size)
            result = product(turned[...], both_all[:, :, f_part(1, j - 1)].reshape(total, 2 * size))
            gate_main[:, f] = result[:, :size]
            up_main[:, f] = result[:, size:]
        return carry

    lax.fori_loop(0, DOWN_AT, main_step, 0)

    @pl.when(out_last)
    def _():
        def take(i, carry):
            out_step(i)
            return carry

        lax.fori_loop(0, n_all, take, 0)
        down_product()

    lax.fori_loop(DOWN_AT, LATE - TAIL + 1, main_step, 0)

    def sent(ref, sem):
        remote(ref, ref, sem, c_recv.at[0], partner, t).wait_send()

    for k in range(rows):
        ups = k + 1
        downs = rows - k

        @pl.when(jnp.logical_and(z == k, has_up))
        def _():
            sent(og.at[:, :ups * cols], u_send)

        @pl.when(jnp.logical_and(z == k, has_down))
        def _():
            sent(og.at[:, :downs * cols], d_send)

    sent(og.at[:, :rows * cols], y_send)

    @pl.when(jnp.logical_not(owned))
    def _():
        sent(li, x_send.at[0])

    @pl.when(crosses)
    def _():
        sent(li, x_send.at[1])

    far_out = xout.at[:n_dp - 2]
    for flag, ref, sem in (
            (in_up, columns, zu_send.at[0]), (in_down, columns, zd_send.at[0]), (in_chain, columns, cy_send.at[0]),
            (out_up, far_out, zu_send.at[1]), (out_down, far_out, zd_send.at[1]),
            (jnp.logical_and(in_chain, at_out_head), xout.at[:n_dp - 2, :, :cols], cy_send.at[1])):
        @pl.when(flag)
        def _():
            sent(ref, sem)

    for a in range(2):
        own = acts[a].at[d]
        sent(own, ac_send.at[a, 0])
        for r in range(1, chips):
            sent(own, ax_send.at[a, r - 1])
            if a == 0:
                sent(own, ac_send.at[0, r])
    for j in range(LATE - TAIL + 1, LATE):
        relay(j)
    for j in range(LATE - TAIL, LATE):
        arrived(j)
    for r in range(1, chips):
        sent(both_all.at[d], ac_send.at[1, r])


def finish(down_in, gate_in, up_in, turned, both_all, down_out, gate_out, up_out, gate_tail, up_tail, sems):
    n_dp, tokens, hidden2 = both_all.shape
    total = n_dp * tokens
    main = gate_in.shape[1]
    size = hidden2 // 2 // LATE
    copies = [
        pltpu.make_async_copy(down_in, down_out, sems.at[0]),
        pltpu.make_async_copy(gate_in, gate_out.at[:, :main], sems.at[1]),
        pltpu.make_async_copy(up_in, up_out.at[:, :main], sems.at[2]),
    ]
    for copy in copies:
        copy.start()
    for j in range(TAIL):
        f = slice(main + j * size, main + (j + 1) * size)
        acts = both_all[:, :, 2 * f.start:2 * f.stop].reshape(total, 2 * size)
        result = jnp.dot(turned[...], acts, preferred_element_type=jnp.float32).astype(jnp.bfloat16)
        gate_tail[j] = result[:, :size]
        up_tail[j] = result[:, size:]
        for k, (tail, out) in enumerate(((gate_tail, gate_out), (up_tail, up_out))):
            copies.append(pltpu.make_async_copy(tail.at[j], out.at[:, f], sems.at[3 + j * 2 + k]))
            copies[-1].start()
    for copy in copies:
        copy.wait()


def shards(n_dp, n_t, out_grad, layer_input, w_down, silu_gate, up_proj, slope_codes):
    hidden, width = w_down.shape
    cols = out_grad.shape[2]
    tokens = out_grad.shape[0] * out_grad.shape[1]
    chips, rows, block = n_dp // 2, n_t // 2, width // n_dp
    words = tokens // 10
    total = n_dp * tokens
    row, col = np.arange(tokens)[:, None], np.arange(tokens)[None, :]
    spread = jnp.asarray(col == (row % 10) * words + row // 10, jnp.bfloat16)
    units = (n_dp + (n_dp - 2) * (n_t // n_dp)) * SPLIT
    far = chips - 1
    bf16 = jnp.bfloat16
    dma = pltpu.SemaphoreType.DMA
    vmem = pl.BlockSpec(memory_space=pltpu.VMEM)
    anywhere = pl.BlockSpec(memory_space=pl.ANY)
    main = hidden // LATE * (LATE - TAIL)
    flops = 2 * tokens * hidden * width + 5 * total * hidden * block
    held = pl.pallas_call(
        functools.partial(exchange, n_dp, n_t),
        out_shape=tuple(pltpu.VMEM(shape, bf16) for shape in (
            (hidden, block), (block, main), (block, main), (block, total),
            (n_dp, tokens, 2 * hidden))),
        in_specs=[anywhere] * 7,
        out_specs=[vmem] * 5,
        scratch_shapes=[
            pltpu.VMEM((tokens, width), bf16),
            pltpu.VMEM((tokens, cols), bf16),
            pltpu.VMEM((tokens, hidden), bf16),
            pltpu.VMEM((tokens, hidden), bf16),
            pltpu.VMEM((words, hidden), jnp.int32),
            pltpu.VMEM((tokens, tokens), bf16),
            pltpu.VMEM((hidden, width), bf16),
            pltpu.VMEM((tokens, hidden), jnp.float32),
            pltpu.VMEM((tokens, hidden), jnp.float32),
            pltpu.VMEM((n_dp, tokens, hidden), bf16),
            pltpu.VMEM((n_dp, tokens, block), bf16),
            pltpu.VMEM((n_dp, tokens, block), bf16),
            dma((6,)), dma, dma, dma, dma((rows, OG_SPLIT)), dma, dma((rows,)),
            dma((2,)), dma((units,)), dma((2,)), dma((2,)), dma((2,)), dma, dma, dma, dma,
            dma((2, far)), dma((2, chips)), dma((far,)), dma, dma((far,)), dma((far, LATE)), dma, dma((far, LATE)),
        ],
        compiler_params=pltpu.CompilerParams(
            collective_id=0, has_side_effects=True, vmem_limit_bytes=38 * 1024 * 1024),
        cost_estimate=pl.CostEstimate(flops=flops, bytes_accessed=20_000_000, transcendentals=0),
    )(
        out_grad.reshape(tokens, cols), layer_input.reshape(tokens, cols),
        silu_gate.reshape(tokens, hidden), up_proj.reshape(tokens, hidden),
        slope_codes.reshape(words, hidden), spread, w_down,
    )
    across = jax.ShapeDtypeStruct((block, hidden), bf16)
    size = hidden // LATE
    return pl.pallas_call(
        finish,
        out_shape=(jax.ShapeDtypeStruct((hidden, block), bf16), across, across),
        in_specs=[vmem] * 5,
        out_specs=[anywhere] * 3,
        scratch_shapes=[
            pltpu.VMEM((TAIL, block, size), bf16), pltpu.VMEM((TAIL, block, size), bf16), dma((3 + 2 * TAIL,))],
        compiler_params=pltpu.CompilerParams(vmem_limit_bytes=12 * 1024 * 1024),
    )(*(pltpu.with_memory_space_constraint(value, pltpu.VMEM) for value in held))


def solution(mesh):
    n_dp, n_t = mesh.shape["dp"], mesh.shape["tensor"]
    return jax.shard_map(
        functools.partial(shards, n_dp, n_t),
        mesh=mesh,
        in_specs=(
            P(None, "dp", "tensor"),
            P(None, "dp", "tensor"),
            P("tensor", None),
            P(None, "dp", "tensor"),
            P(None, "dp", "tensor"),
            P(None, "dp", "tensor"),
        ),
        out_specs=(P("tensor", "dp"), P("dp", "tensor"), P("dp", "tensor")),
        check_vma=False,
    )
```

```python
import functools

import jax
import jax.numpy as jnp
import numpy as np
from jax import lax
from jax.experimental import pallas as pl
from jax.experimental.pallas import tpu as pltpu
from jax.sharding import PartitionSpec as P

SLOPE_LEVELS = (-0.09, 0.06, 0.22, 0.41, 0.6, 0.79, 0.96, 1.08)
MESH = pl.DeviceIdType.MESH
EARLY = 4
HELD = 1
LATE = 8
DOWN_AT = 5
RELAY_AT = 7
THEN = 3
AHEAD = 1
TAIL = 1
OG_SPLIT = 4
SPLIT = 2
IN_PACE = 1
IN_HOP = 3
SIDE_LAG = 2
OUT_PACE = 2
OUT_HOP = 2
WAVE_AT = 0
LAG = 4


def exchange(n_dp, n_t, out_hbm, in_hbm, silu_hbm, up_hbm, code_hbm, spread_hbm, w_hbm,
             down, gate_main, up_main, turned, both_all,
             og, li, silu, up, codes, spread, w, slopes_up, acc, hid_all, xin, xout,
             l_sem, w_sem, u_send, d_send, r_recv, y_send, y_recv,
             x_send, c_recv, zu_send, zd_send, cy_send, cy_recv, o_sem, o_send, o_recv,
             ax_send, ac_send, hx_recv, hc_recv, hp_recv, ax_recv, ac_recv, ap_recv):
    chips = n_dp // 2
    rows = n_t // 2
    ratio = n_t // n_dp
    tokens, cols = out_hbm.shape
    hidden, width = w_hbm.shape
    block = width // n_dp
    part = cols // SPLIT
    fine = min(OG_SPLIT, cols // 128)
    total = n_dp * tokens
    n_in, n_out = n_dp * SPLIT, (n_dp - 2) * SPLIT
    n_all = n_out * ratio
    acts = (hid_all, both_all)
    pieces = (EARLY, LATE)
    size = hidden // LATE

    d = lax.axis_index("dp")
    t = lax.axis_index("tensor")
    q, c = d // 2, lax.rem(d, 2)
    z, y = t // 2, lax.rem(t, 2)
    partner = q * 2 + (1 - c)
    y_peer = z * 2 + (1 - y)
    z_up = lax.min(z + 1, rows - 1) * 2 + y
    z_down = lax.max(z - 1, 0) * 2 + y
    has_up, has_down = z + 1 < rows, z > 0
    owner = t // ratio
    if ratio == 2:
        in_chain = d >= 0
        has_side = d >= 0
        chain_col, side_col = y, 1 - y
    else:
        in_chain = lax.rem(d, 2) == y
        has_side = lax.rem(d, 2) != y
        chain_col, side_col = y * 0, y * 0
    in_head = (d * ratio) // 2
    out_head = lax.rem(in_head + rows // 2, rows)

    def chip_at(r):
        return lax.rem(q + r, chips) * 2 + c

    def group_from(r, core):
        return lax.rem(q + chips - r, chips) * 2 + core

    def span(index, size):
        return pl.ds(pl.multiple_of(index * size, 128), size)

    def remote(src, dst, send, recv, dp, tensor):
        return pltpu.make_async_remote_copy(
            src_ref=src, dst_ref=dst, send_sem=send, recv_sem=recv,
            device_id={"dp": dp, "tensor": tensor}, device_id_type=MESH)

    my_cols = og.at[:, span(t, cols)]
    loads = [
        pltpu.make_async_copy(out_hbm, my_cols, l_sem.at[0]),
        pltpu.make_async_copy(in_hbm, li, l_sem.at[1]),
        pltpu.make_async_copy(silu_hbm, silu, l_sem.at[2]),
        pltpu.make_async_copy(up_hbm, up, l_sem.at[3]),
        pltpu.make_async_copy(code_hbm, codes, l_sem.at[4]),
        pltpu.make_async_copy(spread_hbm, spread, l_sem.at[5]),
    ]
    for load in loads:
        load.start()

    fw = min(512, hidden)

    def w_copy(j):
        f = span(j, fw)
        return pltpu.make_async_copy(w_hbm.at[f], w.at[f], w_sem)

    barrier = pltpu.get_barrier_semaphore()
    greet = [(d, y_peer), (partner, t)]
    greet += [(chip_at(r), t) for r in range(1, chips)]
    for r in range(1, chips):
        greet.append((lax.rem(q + r, chips) * 2 + 1 - c, t))
    for dp, tensor in greet:
        pl.semaphore_signal(barrier, inc=1, device_id={"dp": dp, "tensor": tensor}, device_id_type=MESH)

    @pl.when(has_up)
    def _():
        pl.semaphore_signal(barrier, inc=1, device_id={"dp": d, "tensor": z_up}, device_id_type=MESH)

    @pl.when(has_down)
    def _():
        pl.semaphore_signal(barrier, inc=1, device_id={"dp": d, "tensor": z_down}, device_id_type=MESH)

    at_end = jnp.logical_or(z == 0, z == rows - 1)

    pl.semaphore_wait(barrier, len(greet) + has_up.astype(jnp.int32) + has_down.astype(jnp.int32))

    def og_piece(row, col, h):
        return og.at[:, span((row * 2 + col) * fine + h, cols // fine)]

    def along(row, h, send, tensor):
        piece = og_piece(row, y, h)
        return remote(piece, piece, send, r_recv.at[row, h], d, tensor)

    def up_copy(s, h):
        return along(lax.max(z - s + 1, 0), h, u_send, z_up)

    def down_copy(s, h):
        return along(lax.min(z + s - 1, rows - 1), h, d_send, z_down)

    def up_wait(s, h):
        return along(lax.max(z - s, 0), h, u_send, z_up)

    def down_wait(s, h):
        return along(lax.min(z + s, rows - 1), h, d_send, z_down)

    def across(row, h):
        piece = og_piece(row, y, h)
        return remote(piece, piece, y_send, y_recv.at[row], d, y_peer)

    def across_wait(row):
        piece = og.at[:, span(row * 2 + 1 - y, cols)]
        return remote(piece, piece, y_send, y_recv.at[row], d, y_peer)

    loads[0].wait()

    for h in range(fine):
        across(z, h).start()

        @pl.when(has_up)
        def _():
            up_copy(1, h).start()

        @pl.when(has_down)
        def _():
            down_copy(1, h).start()

    def in_piece(group, col, h):
        return xin.at[group, :, span(col * SPLIT + h, part)]

    def out_piece(group, col, h):
        return xout.at[group, :, span(col * SPLIT + h, part)]

    in_slot = (lax.rem(owner // 2 + chips - q, chips) * 2 + c) * SPLIT

    def li_remote(h):
        return remote(li.at[:, h * part:(h + 1) * part], in_piece(d, chain_col_of(t), h),
                      x_send.at[0], c_recv.at[in_slot + h], owner, t)

    def li_local(h):
        return pltpu.make_async_copy(li.at[:, h * part:(h + 1) * part], in_piece(d, chain_col_of(t), h),
                                     c_recv.at[in_slot + h])

    def chain_col_of(tensor):
        return lax.rem(tensor, 2) if ratio == 2 else tensor * 0

    loads[1].wait()
    owned = owner == d

    @pl.when(owned)
    def _():
        for h in range(SPLIT):
            li_local(h).start()

    @pl.when(jnp.logical_not(owned))
    def _():
        for h in range(SPLIT):
            li_remote(h).start()

    far_row = lax.rem(z + rows // 2, rows)
    far_owner = (far_row * 2 + y) // ratio
    crosses = far_owner // 2 != q
    far_dist = lax.max(lax.rem(far_owner // 2 + chips - q, chips), 1)
    out_slot = n_in + ((far_dist - 1) * 2 + c) * SPLIT

    def og_far(h):
        src = og.at[:, span((far_row * 2 + y) * SPLIT + h, part)]
        return remote(src, out_piece(d, chain_col_of(t), h),
                      x_send.at[1], c_recv.at[out_slot + h], far_owner, t)

    def f_part(a, j):
        return span(j, acts[a].shape[2] // pieces[a])

    def own_chip(a, j, r):
        own = acts[a].at[d, :, f_part(a, j)]
        land = hx_recv.at[r - 1] if a == 0 else ax_recv.at[r - 1, j]
        return remote(own, own, ax_send.at[a, r - 1], land, chip_at(r), t)

    def own_core(a, j):
        own = acts[a].at[d, :, f_part(a, j)]
        return remote(own, own, ac_send.at[a, 0], (ac_recv if a else hc_recv), partner, t)

    def send_own(a, j):
        for r in range(1, chips):
            own_chip(a, j, r).start()
        own_core(a, j).start()

    def chip_hidden(r):
        land = hid_all.at[group_from(r, c)]
        return remote(land, land, ac_send.at[0, r], hx_recv.at[r - 1], partner, t)

    def pass_hidden(r, core):
        land = hid_all.at[group_from(r, core)]
        return remote(land, land, ac_send.at[0, r], hp_recv.at[r - 1], partner, t)

    def chip_late(j, r):
        land = both_all.at[group_from(r, c), :, f_part(1, j)]
        return remote(land, land, ac_send.at[1, r], ax_recv.at[r - 1, j], partner, t)

    def pass_late(j, r, core):
        land = both_all.at[group_from(r, core), :, f_part(1, j)]
        return remote(land, land, ac_send.at[1, r], ap_recv.at[r - 1, j], partner, t)

    def relay(j):
        for r in range(1, chips):
            chip_late(j, r).wait_recv()
            pass_late(j, r, c).start()

    def arrived(j):
        for r in range(1, chips):
            pass_late(j, r, 1 - c).wait_recv()

    loads[2].wait()
    loads[3].wait()
    for j in range(hidden // fw):
        w_copy(j).start()

    def early(j, carry):
        f = f_part(0, j)
        hid_all[d, :, f] = (silu[:, f].astype(jnp.float32) * up[:, f].astype(jnp.float32)).astype(jnp.bfloat16)

        @pl.when(j < EARLY - HELD)
        def _():
            send_own(0, j)
        return carry

    lax.fori_loop(0, EARLY, early, 0)

    loads[4].wait()
    loads[5].wait()
    acc[...] = jnp.zeros_like(acc)

    def decode(j, carry):
        f = span(j, fw)
        words = codes[:, f]
        symbols = jnp.dot(
            spread[...],
            jnp.concatenate([((words >> (3 * k)) & 7).astype(jnp.float32).astype(jnp.bfloat16) for k in range(10)], axis=0),
            preferred_element_type=jnp.float32)
        slopes = jnp.full(symbols.shape, SLOPE_LEVELS[0], jnp.float32)
        for s in range(1, 8):
            slopes = jnp.where(symbols > s - 0.5, jnp.float32(SLOPE_LEVELS[s]), slopes)
        slopes_up[:, f] = up[:, f].astype(jnp.float32) * slopes
        return carry

    lax.fori_loop(0, hidden // fw, decode, 0)

    def unit(i):
        h, u = lax.rem(i, SPLIT), i // SPLIT
        return lax.rem(u, 2), u // 2, h

    def in_ref(i, col):
        core, r, h = unit(i)
        return in_piece(group_from(r, core), col, h)

    def in_copies(i):
        piece = in_ref(i, chain_col)
        return (remote(piece, piece, zu_send.at[0], c_recv.at[i], d, z_up),
                remote(piece, piece, zd_send.at[0], c_recv.at[i], d, z_down),
                remote(piece, piece, cy_send.at[0], cy_recv, d, y_peer))

    in_up = jnp.logical_and(in_chain, jnp.logical_and(z >= in_head, has_up))
    in_down = jnp.logical_and(in_chain, jnp.logical_and(z <= in_head, has_down))

    def in_rows(i):
        up_next, down_next, side = in_copies(i)
        up_next.wait_recv()

        @pl.when(in_up)
        def _():
            up_next.start()

        @pl.when(in_down)
        def _():
            down_next.start()

    def head_wait(i, carry):
        in_copies(i)[0].wait_recv()
        return carry

    def head_up(i, carry):
        in_copies(i)[0].start()
        return carry

    def head_down(i, carry):
        in_copies(i)[1].start()
        return carry

    def in_side(i, carry):
        in_copies(i)[2].start()
        return carry

    out_up = jnp.logical_and(z >= out_head, has_up)
    out_down = jnp.logical_and(z <= out_head, has_down)
    at_out_head = z == out_head

    in_far = lax.max(z - in_head, in_head - z)
    out_far = lax.max(z - out_head, out_head - z)
    out_last = jnp.logical_and(at_end, out_far > jnp.where(in_chain, in_far, 0))

    def out_step(i):
        if ratio == 2:
            native, other = i < n_out, i + n_out
            col = jnp.where(native, y, 1 - y)
        else:
            native, other, col = in_chain, i, y * 0
        core, r, h = unit(lax.rem(i, n_out))
        piece = out_piece(group_from(r + 1, core), col, h)
        n = n_in + i
        up_next = remote(piece, piece, zu_send.at[1], c_recv.at[n], d, z_up)
        down_next = remote(piece, piece, zd_send.at[1], c_recv.at[n], d, z_down)
        side = remote(piece, piece, cy_send.at[1], c_recv.at[n_in + lax.min(other, n_all - 1)], d, y_peer)
        up_next.wait_recv()

        @pl.when(jnp.logical_and(native, at_out_head))
        def _():
            side.start()

        @pl.when(out_up)
        def _():
            up_next.start()

        @pl.when(out_down)
        def _():
            down_next.start()

    at_in_head = jnp.logical_and(in_chain, in_far == 0)

    def matmul_piece(piece):
        k = span(piece, cols)
        acc[...] += lax.dot_general(og[:, k], w[:, k], (((1,), (1,)), ((), ())),
                                    preferred_element_type=jnp.float32)

    def wave_step(s):
        past = jnp.logical_and(in_chain, in_far > 0)
        first = IN_PACE * (s - IN_HOP * (in_far - 1))
        for i in range(IN_PACE):
            @pl.when(jnp.logical_and(past, jnp.logical_and(first + i >= 0, first + i < n_in)))
            def _():
                in_rows(first + i)

        late_side = first - IN_PACE * SIDE_LAG
        for i in range(IN_PACE):
            @pl.when(jnp.logical_and(past, jnp.logical_and(late_side + i >= 0, late_side + i < n_in)))
            def _():
                in_side(late_side + i, 0)

        out_first = OUT_PACE * (s - LAG - OUT_HOP * out_far)
        for i in range(OUT_PACE):
            @pl.when(jnp.logical_and(jnp.logical_not(out_last), jnp.logical_and(out_first + i >= 0, out_first + i < n_all)))
            def _():
                out_step(out_first + i)

    order, place = [], 0
    for dist in range(rows + 1):
        for far_side in (0, 1):
            away = dist - far_side
            for way in ((-1, 1) if away > 0 else (1,) if away == 0 else ()):
                row = z + way * away
                valid = jnp.logical_and(row >= 0, row < rows)
                order.append((valid, place, row, far_side))
                place = place + valid.astype(jnp.int32)

    def multiply(p):
        row, side = 0, 0
        for valid, place, its_row, far_side in order:
            mine = jnp.logical_and(valid, place == p)
            row = jnp.where(mine, its_row, row)
            side = jnp.where(mine, far_side, side)

        @pl.when(side == 1)
        def _():
            across_wait(row).wait_recv()

        matmul_piece(row * 2 + jnp.where(side == 1, 1 - y, y))

    arrivals = fine * (rows - 1)

    def gather(e, carry):
        s, h = e // fine + 1, lax.rem(e, fine)
        last_part = h == fine - 1

        @pl.when(z >= s)
        def _():
            up_wait(s, h).wait_recv()

            @pl.when(has_up)
            def _():
                up_copy(s + 1, h).start()

            across(lax.max(z - s, 0), h).start()

        @pl.when(z + s < rows)
        def _():
            down_wait(s, h).wait_recv()

            @pl.when(has_down)
            def _():
                down_copy(s + 1, h).start()

            across(lax.min(z + s, rows - 1), h).start()

        @pl.when(jnp.logical_and(s == rows // 2, last_part))
        def _():
            @pl.when(crosses)
            def _():
                for k in range(SPLIT):
                    og_far(k).start()

            for j in range(EARLY - HELD, EARLY):
                send_own(0, j)

        @pl.when(at_in_head)
        def _():
            @pl.when(e == fine - 1)
            def _():
                lax.fori_loop(near, n_in, head_wait, 0)

            @pl.when(jnp.logical_and(in_up, e == fine * lax.max(z, 1) - 1))
            def _():
                lax.fori_loop(jnp.where(z == 0, near, 0), n_in, head_up, 0)

            @pl.when(jnp.logical_and(in_down, e == fine * lax.max(rows - 1 - z, 1) - 1))
            def _():
                lax.fori_loop(jnp.where(z == rows - 1, near, 0), n_in, head_down, 0)

            @pl.when(e == arrivals - 1)
            def _():
                lax.fori_loop(0, n_in, in_side, 0)

        @pl.when(e == fine - 1)
        def _():
            pltpu.make_async_copy(w_hbm, w, w_sem).wait()

        pace = max(fine // 2, 1)
        p = jnp.where(e < arrivals, (e + 1) // pace - 2, e - arrivals + arrivals // pace - 1)
        now = jnp.logical_and(p >= 0, jnp.logical_or(e >= arrivals, lax.rem(e + 1, pace) == 0))

        @pl.when(jnp.logical_and(now, p >= 3 + WAVE_AT))
        def _():
            wave_step(p - 3 - WAVE_AT)

        @pl.when(now)
        def _():
            multiply(p)
        return carry

    near = 2 * SPLIT

    @pl.when(at_in_head)
    def _():
        lax.fori_loop(0, near, head_wait, 0)

        @pl.when(z == 0)
        def _():
            lax.fori_loop(0, near, head_up, 0)

        @pl.when(z == rows - 1)
        def _():
            lax.fori_loop(0, near, head_down, 0)

    lax.fori_loop(0, arrivals + n_t - arrivals // max(fine // 2, 1) + 1, gather, 0)

    o_own = pltpu.make_async_copy(og.at[:, span(d, block)], xout.at[d], o_sem)
    o_own.start()
    o_other = remote(og.at[:, span(partner, block)], xout.at[d], o_send, o_recv, partner, t)
    o_other.start()

    def late(j, carry):
        f = span(j, size)
        grad = acc[:, f]
        both_all[d, :, span(2 * j, size)] = (grad * slopes_up[:, f]).astype(jnp.bfloat16)
        both_all[d, :, span(2 * j + 1, size)] = (grad * silu[:, f].astype(jnp.float32)).astype(jnp.bfloat16)
        send_own(1, j)
        return carry

    lax.fori_loop(0, LATE, late, 0)

    steps = max(-(-n_in // IN_PACE) + SIDE_LAG + IN_HOP * (rows - 2), -(-n_all // OUT_PACE) + LAG + OUT_HOP * (rows - 1))

    def wave(s, carry):
        @pl.when(s == RELAY_AT)
        def _():
            for r in range(1, chips):
                chip_hidden(r).wait_recv()
                pass_hidden(r, c).start()

        wave_step(s)
        return carry

    lax.fori_loop(n_t - 3 - WAVE_AT, steps, wave, 0)

    def late_relay(j, carry):
        relay(j)
        return carry

    lax.fori_loop(0, AHEAD, late_relay, 0)

    def product(left, right):
        return jnp.dot(left, right, preferred_element_type=jnp.float32).astype(jnp.bfloat16)

    def down_product():
        o_own.wait()
        o_other.wait()
        theirs = hid_all.at[partner]
        remote(theirs, theirs, ac_send.at[0, 0], hc_recv, partner, t).wait_recv()
        for r in range(1, chips):
            pass_hidden(r, 1 - c).wait_recv()

        def down_step(j, carry):
            f = span(j, fw)
            down[f, :] = product(hid_all[:, :, f].reshape(total, fw).T, xout[...].reshape(total, block))
            return carry

        lax.fori_loop(0, hidden // fw, down_step, 0)

    @pl.when(jnp.logical_not(out_last))
    def _():
        down_product()

    lax.fori_loop(AHEAD, THEN, late_relay, 0)
    columns = xin.at[:, :, :cols]

    @pl.when(has_side)
    def _():
        remote(columns, columns, cy_send.at[0], cy_recv, d, y_peer).wait_recv()

    turned[...] = xin[...].reshape(total, block).T
    theirs_late = both_all.at[partner]
    remote(theirs_late, theirs_late, ac_send.at[1, 0], ac_recv, partner, t).wait_recv()

    def main_step(j, carry):
        @pl.when(j >= THEN)
        def _():
            relay(j)

        @pl.when(j > 0)
        def _():
            arrived(j - 1)
            f = span(j - 1, size)
            result = product(turned[...], both_all[:, :, f_part(1, j - 1)].reshape(total, 2 * size))
            gate_main[:, f] = result[:, :size]
            up_main[:, f] = result[:, size:]
        return carry

    lax.fori_loop(0, DOWN_AT, main_step, 0)

    @pl.when(out_last)
    def _():
        def take(i, carry):
            out_step(i)
            return carry

        lax.fori_loop(0, n_all, take, 0)
        down_product()

    lax.fori_loop(DOWN_AT, LATE - TAIL + 1, main_step, 0)

    def sent(ref, sem):
        remote(ref, ref, sem, c_recv.at[0], partner, t).wait_send()

    for k in range(rows):
        ups = k + 1
        downs = rows - k

        @pl.when(jnp.logical_and(z == k, has_up))
        def _():
            sent(og.at[:, :ups * cols], u_send)

        @pl.when(jnp.logical_and(z == k, has_down))
        def _():
            sent(og.at[:, :downs * cols], d_send)

    sent(og.at[:, :rows * cols], y_send)

    @pl.when(jnp.logical_not(owned))
    def _():
        sent(li, x_send.at[0])

    @pl.when(crosses)
    def _():
        sent(li, x_send.at[1])

    far_out = xout.at[:n_dp - 2]
    for flag, ref, sem in (
            (in_up, columns, zu_send.at[0]), (in_down, columns, zd_send.at[0]), (in_chain, columns, cy_send.at[0]),
            (out_up, far_out, zu_send.at[1]), (out_down, far_out, zd_send.at[1]),
            (jnp.logical_and(in_chain, at_out_head), xout.at[:n_dp - 2, :, :cols], cy_send.at[1])):
        @pl.when(flag)
        def _():
            sent(ref, sem)

    for a in range(2):
        own = acts[a].at[d]
        sent(own, ac_send.at[a, 0])
        for r in range(1, chips):
            sent(own, ax_send.at[a, r - 1])
            if a == 0:
                sent(own, ac_send.at[0, r])
    for j in range(LATE - TAIL + 1, LATE):
        relay(j)
    for j in range(LATE - TAIL, LATE):
        arrived(j)
    for r in range(1, chips):
        sent(both_all.at[d], ac_send.at[1, r])


def finish(down_in, gate_in, up_in, turned, both_all, down_out, gate_out, up_out, gate_tail, up_tail, sems):
    n_dp, tokens, hidden2 = both_all.shape
    total = n_dp * tokens
    main = gate_in.shape[1]
    size = hidden2 // 2 // LATE
    copies = [
        pltpu.make_async_copy(down_in, down_out, sems.at[0]),
        pltpu.make_async_copy(gate_in, gate_out.at[:, :main], sems.at[1]),
        pltpu.make_async_copy(up_in, up_out.at[:, :main], sems.at[2]),
    ]
    for copy in copies:
        copy.start()
    for j in range(TAIL):
        f = slice(main + j * size, main + (j + 1) * size)
        acts = both_all[:, :, 2 * f.start:2 * f.stop].reshape(total, 2 * size)
        result = jnp.dot(turned[...], acts, preferred_element_type=jnp.float32).astype(jnp.bfloat16)
        gate_tail[j] = result[:, :size]
        up_tail[j] = result[:, size:]
        for k, (tail, out) in enumerate(((gate_tail, gate_out), (up_tail, up_out))):
            copies.append(pltpu.make_async_copy(tail.at[j], out.at[:, f], sems.at[3 + j * 2 + k]))
            copies[-1].start()
    for copy in copies:
        copy.wait()


def shards(n_dp, n_t, out_grad, layer_input, w_down, silu_gate, up_proj, slope_codes):
    hidden, width = w_down.shape
    cols = out_grad.shape[2]
    tokens = out_grad.shape[0] * out_grad.shape[1]
    chips, rows, block = n_dp // 2, n_t // 2, width // n_dp
    words = tokens // 10
    total = n_dp * tokens
    row, col = np.arange(tokens)[:, None], np.arange(tokens)[None, :]
    spread = jnp.asarray(col == (row % 10) * words + row // 10, jnp.bfloat16)
    units = (n_dp + (n_dp - 2) * (n_t // n_dp)) * SPLIT
    far = chips - 1
    bf16 = jnp.bfloat16
    dma = pltpu.SemaphoreType.DMA
    vmem = pl.BlockSpec(memory_space=pltpu.VMEM)
    anywhere = pl.BlockSpec(memory_space=pl.ANY)
    main = hidden // LATE * (LATE - TAIL)
    flops = 2 * tokens * hidden * width + 5 * total * hidden * block
    held = pl.pallas_call(
        functools.partial(exchange, n_dp, n_t),
        out_shape=tuple(pltpu.VMEM(shape, bf16) for shape in (
            (hidden, block), (block, main), (block, main), (block, total),
            (n_dp, tokens, 2 * hidden))),
        in_specs=[anywhere] * 7,
        out_specs=[vmem] * 5,
        scratch_shapes=[
            pltpu.VMEM((tokens, width), bf16),
            pltpu.VMEM((tokens, cols), bf16),
            pltpu.VMEM((tokens, hidden), bf16),
            pltpu.VMEM((tokens, hidden), bf16),
            pltpu.VMEM((words, hidden), jnp.int32),
            pltpu.VMEM((tokens, tokens), bf16),
            pltpu.VMEM((hidden, width), bf16),
            pltpu.VMEM((tokens, hidden), jnp.float32),
            pltpu.VMEM((tokens, hidden), jnp.float32),
            pltpu.VMEM((n_dp, tokens, hidden), bf16),
            pltpu.VMEM((n_dp, tokens, block), bf16),
            pltpu.VMEM((n_dp, tokens, block), bf16),
            dma((6,)), dma, dma, dma, dma((rows, OG_SPLIT)), dma, dma((rows,)),
            dma((2,)), dma((units,)), dma((2,)), dma((2,)), dma((2,)), dma, dma, dma, dma,
            dma((2, far)), dma((2, chips)), dma((far,)), dma, dma((far,)), dma((far, LATE)), dma, dma((far, LATE)),
        ],
        compiler_params=pltpu.CompilerParams(
            collective_id=0, has_side_effects=True, vmem_limit_bytes=38 * 1024 * 1024),
        cost_estimate=pl.CostEstimate(flops=flops, bytes_accessed=20_000_000, transcendentals=0),
    )(
        out_grad.reshape(tokens, cols), layer_input.reshape(tokens, cols),
        silu_gate.reshape(tokens, hidden), up_proj.reshape(tokens, hidden),
        slope_codes.reshape(words, hidden), spread, w_down,
    )
    across = jax.ShapeDtypeStruct((block, hidden), bf16)
    size = hidden // LATE
    return pl.pallas_call(
        finish,
        out_shape=(jax.ShapeDtypeStruct((hidden, block), bf16), across, across),
        in_specs=[vmem] * 5,
        out_specs=[anywhere] * 3,
        scratch_shapes=[
            pltpu.VMEM((TAIL, block, size), bf16), pltpu.VMEM((TAIL, block, size), bf16), dma((3 + 2 * TAIL,))],
        compiler_params=pltpu.CompilerParams(vmem_limit_bytes=12 * 1024 * 1024),
    )(*(pltpu.with_memory_space_constraint(value, pltpu.VMEM) for value in held))


def solution(mesh):
    n_dp, n_t = mesh.shape["dp"], mesh.shape["tensor"]
    return jax.shard_map(
        functools.partial(shards, n_dp, n_t),
        mesh=mesh,
        in_specs=(
            P(None, "dp", "tensor"),
            P(None, "dp", "tensor"),
            P("tensor", None),
            P(None, "dp", "tensor"),
            P(None, "dp", "tensor"),
            P(None, "dp", "tensor"),
        ),
        out_specs=(P("tensor", "dp"), P("dp", "tensor"), P("dp", "tensor")),
        check_vma=False,
    )
```
